8 devices in a mesh: dp: 1 (over z), tp: 8 (over x, y, core).
Axes of the slice: x: 2, y: 2, z: 1, core: 2. Of those that a mesh axis runs over, the one named last changes fastest.
Arguments:
- x: bfloat16 [4096, 2048], P(('dp', 'tp'))
- gain: bfloat16 [2048], replicated
- wq: bfloat16 [2048, 4096], P(None, 'tp')
- wk: bfloat16 [2048, 2048], P(None, 'tp')
- wv: bfloat16 [2048, 2048], P(None, 'tp')
- wo: bfloat16 [4096, 2048], P('tp')
Outputs:
- output: bfloat16 [4096, 2048], P(('dp', 'tp'))
All inputs are finite; a program needn't handle non-finite values.
Results may differ from the reference program's by a relative error of at most 0.012.
Values are sent between devices in bfloat16 or wider.
A program may use at most 2 GiB of HBM per device.

```python
import jax
import jax.numpy as jnp
from jax import lax

ROWS = 4096
D = 2048
HEADS = 32
KV_HEADS = 16
HEAD = 128
THETA = 10000


def setup_inputs(seed: int = 0, part: int = 0) -> dict:
    kx, kn, kq, kk, kv, ko = jax.random.split(jax.random.key(seed), 6)

    def weights(key, rows, columns):
        return jax.random.normal(key, (rows, columns), jnp.float32) * rows**-0.5

    drawn = {
        "x": jax.random.normal(jax.random.fold_in(kx, part), (ROWS, D), jnp.float32),
        "gain": 1 + 0.1 * jax.random.normal(kn, (D,), jnp.float32),
        "wq": 2 * weights(kq, D, HEADS * HEAD),
        "wk": 2 * weights(kk, D, KV_HEADS * HEAD),
        "wv": 4 * weights(kv, D, KV_HEADS * HEAD),
        "wo": weights(ko, HEADS * HEAD, D),
    }
    return {k: v.astype(jnp.bfloat16) for k, v in drawn.items()}


def normed(x, gain):
    wide = x.astype(jnp.float32)
    scale = lax.rsqrt(jnp.mean(wide * wide, -1, keepdims=True) + 1e-6)
    return (wide * scale * gain.astype(jnp.float32)).astype(jnp.bfloat16)


def turned(t, place, theta):
    half = t.shape[-1] // 2
    angle = place.astype(jnp.float32)[:, None] * theta ** (-jnp.arange(half, dtype=jnp.float32) / half)
    cos, sin = jnp.cos(angle)[:, None], jnp.sin(angle)[:, None]
    a, b = t[..., :half].astype(jnp.float32), t[..., half:].astype(jnp.float32)
    return jnp.concatenate([a * cos - b * sin, b * cos + a * sin], -1).astype(jnp.bfloat16)


def matmul(a, w):
    return jnp.dot(a, w, preferred_element_type=jnp.float32).astype(jnp.bfloat16)


def einsum(form, a, b):
    return jnp.einsum(form, a.astype(jnp.float32), b.astype(jnp.float32))


def attention(q, k, v):
    scores = einsum("tgsd,ugd->gstu", q, k) * q.shape[-1] ** -0.5
    token = jnp.arange(q.shape[0])
    scores = jnp.where(token[:, None] >= token, scores, -jnp.inf)
    weights = jax.nn.softmax(scores, -1).astype(jnp.bfloat16)
    return einsum("gstu,ugd->tgsd", weights, v).astype(jnp.bfloat16)


def reference(x, gain, wq, wk, wv, wo):
    a, place = normed(x, gain), jnp.arange(ROWS)
    q = turned(matmul(a, wq).reshape(ROWS, HEADS, HEAD), place, THETA).reshape(ROWS, KV_HEADS, -1, HEAD)
    k = turned(matmul(a, wk).reshape(ROWS, KV_HEADS, HEAD), place, THETA)
    v = matmul(a, wv).reshape(ROWS, KV_HEADS, HEAD)
    seen = attention(q, k, v).reshape(ROWS, HEADS * HEAD)
    return (x.astype(jnp.float32) + jnp.dot(seen, wo, preferred_element_type=jnp.float32)).astype(jnp.bfloat16)
```

```python
import functools

import jax
import jax.numpy as jnp
import numpy as np
from jax import lax
from jax.experimental import pallas as pl
from jax.experimental.pallas import tpu as pltpu
from jax.sharding import PartitionSpec as P

HEAD = 128
THETA = 10000
NEG = -1e30
HIDDEN = 2 * NEG
LOG2E = 1.4426950408889634
E = HEAD**-0.5 * LOG2E
UNIT = 256
PIECE = 128
BK = 512
F32, BF16 = jnp.float32, jnp.bfloat16

ORDER = [(1, 1, 0), (1, 1, 2), (1, 0, 0), (0, 1, 2), (1, 1, 1), (1, 1, 3), (1, 0, 1), (0, 1, 3),
         (1, 0, 2), (0, 1, 0), (1, 0, 3), (0, 1, 1), (0, 0, 2), (0, 0, 0), (0, 0, 3), (0, 0, 1)]
LANDING = [(0, 0, 0, 0), (0, 0, 0, 1), (0, 0, 1, 0), (0, 0, 1, 1),
           (0, 1, 0, 0), (1, 0, 0, 1), (0, 1, 1, 0), (1, 0, 1, 1),
           (0, 1, 0, 1), (1, 0, 0, 0), (0, 1, 1, 1), (1, 0, 1, 0),
           (1, 1, 0, 0), (1, 1, 0, 1), (1, 1, 1, 0), (1, 1, 1, 1)]


def _pick(i, table):
    out = jnp.int32(0)
    for n, value in enumerate(table):
        if value:
            out = out + jnp.where(i == n, jnp.int32(value), jnp.int32(0))
    return out


def _flip(bit, by):
    return bit + by - 2 * bit * by


def _dot(a, b, ca=1, cb=0):
    return lax.dot_general(a, b, (((ca,), (cb,)), ((), ())), preferred_element_type=F32)


def _kernel(x_hbm, gain_ref, wq_hbm, wk_hbm, wv_hbm, wo_hbm, coarse_ref, fine_ref, out_ref,
            x_s, wq_s, wk_s, wv_s, wo_s, xg, q_s, k_s, v_s, near_s, far_s, mine_s, o_s, top_s, mix_s,
            load_sem, got_sem, core_sem, xs_sem, ys_sem, near_send, near_got, far_send, far_got):
    me = lax.axis_index("tp")
    mx, my, mc = me // 4, (me // 2) % 2, me % 2
    partner, nx, ny = me + 1 - 2 * mc, me + 4 - 8 * mx, me + 2 - 4 * my

    loads = [pltpu.make_async_copy(a, b, load_sem.at[n])
             for n, (a, b) in enumerate([(x_hbm, x_s), (wq_hbm, wq_s), (wk_hbm, wk_s), (wv_hbm, wv_s), (wo_hbm, wo_s)])]
    for load in loads:
        load.start()
    barrier = pltpu.get_barrier_semaphore()
    for other in (partner, nx, ny):
        pl.semaphore_signal(barrier, inc=1, device_id={"tp": other}, device_id_type=pl.DeviceIdType.MESH)
    pl.semaphore_wait(barrier, 3)
    loads[0].wait()

    def slot(i, rows):
        return xg.at[pl.ds(pl.multiple_of(i * rows, rows), rows), :]

    def remote(src, dst, send, recv, to):
        return pltpu.make_async_remote_copy(src_ref=src, dst_ref=dst, send_sem=send, recv_sem=recv, device_id={"tp": to},
                                            device_id_type=pl.DeviceIdType.MESH)

    def block_to(u, v, sems, to):
        return remote(slot(u, UNIT), slot(v, UNIT), sems.at[u], got_sem.at[v], to)

    gain = gain_ref[...].astype(F32)

    def norm(i, carry):
        at = pl.ds(pl.multiple_of(i * 32, 32), 32)
        wide = x_s[at, :].astype(F32)
        scale = lax.rsqrt(jnp.mean(wide * wide, -1, keepdims=True) + 1e-6)
        xg[at, :] = (wide * scale * gain).astype(BF16)
        return carry

    lax.fori_loop(0, UNIT // 32, norm, 0)
    block_to(0, 4, ys_sem, ny).start()
    block_to(0, 2, core_sem, partner).start()
    lax.fori_loop(UNIT // 32, 2 * UNIT // 32, norm, 0)
    block_to(1, 9, xs_sem, nx).start()
    block_to(0, 8, xs_sem, nx).start()
    block_to(1, 5, ys_sem, ny).start()
    block_to(1, 3, core_sem, partner).start()
    for i in range(2):
        v_s[i, HEAD:, :] = jnp.ones((8, v_s.shape[2]), BF16)
    for load in loads[1:]:
        load.wait()

    sign = jnp.where(lax.broadcasted_iota(jnp.int32, (1, HEAD), 1) < HEAD // 2, -1.0, 1.0).astype(F32)

    def landed(n, carry):
        bx, by, bc, half = (_pick(n, [row[k] for row in LANDING]) for k in range(4))
        u = 8 * bx + 4 * by + 2 * bc + half

        @pl.when(bx + by + bc > 0)
        def _():
            block_to(u, u, core_sem, partner).wait_recv()

        @pl.when((bc == 0) & (bx + by > 0))
        def _():
            block_to(u, u + 2, core_sem, partner).start()

        @pl.when((bc == 0) & (by == 1) & (bx == 0) & (half == 0))
        def _():
            block_to(u, 12, xs_sem, nx).start()

        @pl.when((bc == 0) & (by == 0) & (bx == 1) & (half == 1))
        def _():
            block_to(u, 13, ys_sem, ny).start()

        place = (4 * _flip(mx, bx) + 2 * _flip(my, by) + _flip(mc, bc)) * 2 + half
        rows = pl.ds(pl.multiple_of(place * UNIT, UNIT), UNIT)
        base = coarse_ref[pl.ds(place, 1), :]
        cos_a, sin_a = base[:, :HEAD], base[:, HEAD:]
        cos_b, sin_b = fine_ref[:, :HEAD], fine_ref[:, HEAD:]
        cos = cos_a * cos_b - sin_a * sin_b
        sin = (sin_a * cos_b + cos_a * sin_b) * sign

        def turned(t):
            t = t.astype(BF16).astype(F32)
            return (t * cos + pltpu.roll(t, HEAD // 2, 1) * sin).astype(BF16)

        a = slot(u, UNIT)
        q = _dot(a[...], wq_s[...])
        for i in range(4):
            q_s[i, rows, :] = turned(q[:, i * HEAD : (i + 1) * HEAD])
        k = _dot(a[...], wk_s[...])
        for i in range(2):
            k_s[i, rows, :] = turned(k[:, i * HEAD : (i + 1) * HEAD])
        v = _dot(a[...], wv_s[...])
        for i in range(2):
            v_s[i, :HEAD, rows] = v[:, i * HEAD : (i + 1) * HEAD].T.astype(BF16)
        return carry

    lax.fori_loop(0, 16, landed, 0)
    for u in (0, 1, 4, 5, 8, 9, 12, 13):
        block_to(u, u + 2, core_sem, partner).wait_send()
    for u in (0, 1, 4):
        block_to(u, u, xs_sem, nx).wait_send()
    for u in (0, 1, 9):
        block_to(u, u, ys_sem, ny).wait_send()

    strips = [(i, g) for g in range(2) for i in range(2)]
    strip_of = {s: n for n, s in enumerate(strips)}

    def which(t):
        return tuple(_pick(t, [row[k] for row in ORDER]) for k in range(3))

    def block(first, j, p, todo):
        keys = pl.ds(pl.multiple_of(j * BK, BK), BK)
        scores = []
        for i, g, _ in todo:
            rows = pl.ds(pl.multiple_of(first + g * 512, PIECE), PIECE)
            q = q_s[2 * i : 2 * i + 2, rows, :].reshape(2 * PIECE, HEAD)
            scores.append(_dot(k_s[i, keys, :], q, 1, 1))
        ok = None
        if any(m for _, _, m in todo):
            gap = (lax.broadcasted_iota(jnp.int32, (BK, 2 * PIECE), 1) % PIECE) - lax.broadcasted_iota(jnp.int32, (BK, 2 * PIECE), 0)
            ok = gap + p * PIECE >= 0
        weights, keeps = [], []
        for (i, g, masked), s in zip(todo, scores):
            n = strip_of[i, g]
            if masked:
                s = jnp.where(ok, s, HIDDEN)
            old = top_s[n : n + 1, :]
            top = jnp.maximum(old, s.max(axis=0, keepdims=True))
            top_s[n : n + 1, :] = top
            weights.append(jnp.exp2((s - top) * E).astype(BF16))
            keeps.append(jnp.exp2((old - top) * E))
        for (i, g, _), w, keep in zip(todo, weights, keeps):
            n = strip_of[i, g]
            mix_s[n] = mix_s[n] * keep + _dot(v_s[i, :, keys], w)

    def attend(t):
        bx, by, p = which(t)
        chip = 2 * _flip(mx, bx) + _flip(my, by)
        first = chip * 1024 + p * PIECE
        top_s[...] = jnp.full(top_s.shape, NEG, F32)
        mix_s[...] = jnp.zeros(mix_s.shape, F32)

        def whole(j, carry):
            block(first, j, p, [(i, g, False) for i, g in strips])
            return carry

        lax.fori_loop(0, 2 * chip, whole, 0)
        block(first, 2 * chip, p, [(i, g, g == 0) for i, g in strips])
        block(first, 2 * chip + 1, p, [(i, g, True) for i, g in strips if g == 1])
        for n, (i, g) in enumerate(strips):
            o = (mix_s[n, :HEAD, :] * (1 / mix_s[n, HEAD : HEAD + 1, :])).T.astype(BF16)
            for m in range(2):
                o_s[g, :, (2 * i + m) * HEAD : (2 * i + m + 1) * HEAD] = o[m * PIECE : (m + 1) * PIECE, :]

    def near(t):
        return remote(slot(16 + t, PIECE), near_s.at[t], near_send.at[t], near_got.at[t], partner)

    def far(t, to_slot, to):
        return remote(slot(t, PIECE), far_s.at[to_slot], far_send.at[t], far_got.at[to_slot], to)

    def project(t):
        for n in range(0, 2048, 512):
            slot(16 + t, PIECE)[:, n : n + 512] = _dot(o_s[1 - mc], wo_s[:, n : n + 512]).astype(BF16)
        near(t).start()
        for n in range(0, 2048, 512):
            mine_s[:, n : n + 512] = _dot(o_s[mc], wo_s[:, n : n + 512])

    def finish(t):
        bx, by, p = which(t)
        near(t).wait_recv()
        own = bx + by == 0
        summed = (bx + by == 1) & (((bx == 1) & (p >= 2)) | ((by == 1) & (p < 2)))
        low = p // 2 == 0

        def tiles(body):
            def step(i, carry):
                body(pl.ds(pl.multiple_of(i * 32, 32), 32), i)
                return carry

            lax.fori_loop(0, PIECE // 32, step, 0)

        @pl.when(own)
        def _():
            far(0, 4 + p, nx).wait_recv()
            far(0, 8 + p, ny).wait_recv()

            def body(at, i):
                to = pl.ds(pl.multiple_of(p * PIECE + i * 32, 32), 32)
                total = mine_s[at, :] + near_s[t, at, :].astype(F32)
                total = total + far_s[4 + p, at, :].astype(F32) + far_s[8 + p, at, :].astype(F32)
                out_ref[to, :] = (x_s[to, :].astype(F32) + total).astype(BF16)

            tiles(body)

        @pl.when(summed)
        def _():
            far(0, p, nx).wait_recv()

            def body(at, i):
                to = pl.ds(pl.multiple_of(t * PIECE + i * 32, 32), 32)
                total = mine_s[at, :] + near_s[t, at, :].astype(F32) + far_s[p, at, :].astype(F32)
                xg[to, :] = total.astype(BF16)

            tiles(body)

        @pl.when(jnp.logical_not(own | summed))
        def _():
            def body(at, i):
                to = pl.ds(pl.multiple_of(t * PIECE + i * 32, 32), 32)
                xg[to, :] = (mine_s[at, :] + near_s[t, at, :].astype(F32)).astype(BF16)

            tiles(body)

        to_slot = p + 4 * bx * (1 - by) + 8 * by * (1 - bx)
        along_x = ((bx == 1) & (by == 0)) | ((bx + by == 2) & low)

        @pl.when(jnp.logical_not(own) & along_x)
        def _():
            far(t, to_slot, nx).start()

        @pl.when(jnp.logical_not(own) & jnp.logical_not(along_x))
        def _():
            far(t, to_slot, ny).start()

    def piece(t, carry):
        attend(t)

        @pl.when(t > 0)
        def _():
            finish(t - 1)

        project(t)
        return carry

    lax.fori_loop(0, 16, piece, 0)
    finish(15)

    def sent(t, carry):
        near(t).wait_send()

        @pl.when(t < 12)
        def _():
            far(t, 0, nx).wait_send()

        return carry

    lax.fori_loop(0, 16, sent, 0)


def tables():
    half = HEAD // 2
    rate = np.concatenate([float(THETA) ** (-np.arange(half) / half)] * 2)
    a = np.arange(16)[:, None] * UNIT * rate
    b = np.arange(UNIT)[:, None] * rate
    both = lambda t: np.concatenate([np.cos(t), np.sin(t)], 1).astype(np.float32)
    return both(a), both(b)


def solution(mesh):
    def step(x, gain, wq, wk, wv, wo):
        rows, d = x.shape
        group = rows * 8
        coarse, fine = tables()
        hbm, vmem = pl.BlockSpec(memory_space=pl.ANY), pl.BlockSpec(memory_space=pltpu.VMEM)
        dma = pltpu.SemaphoreType.DMA
        return pl.pallas_call(
            _kernel,
            out_shape=jax.ShapeDtypeStruct((rows, d), BF16),
            in_specs=[hbm, vmem, hbm, hbm, hbm, hbm, vmem, vmem],
            out_specs=vmem,
            scratch_shapes=[
                pltpu.VMEM(x.shape, BF16), pltpu.VMEM(wq.shape, BF16), pltpu.VMEM(wk.shape, BF16), pltpu.VMEM(wv.shape, BF16),
                pltpu.VMEM(wo.shape, BF16),
                pltpu.VMEM((group, d), BF16),
                pltpu.VMEM((4, group, HEAD), BF16), pltpu.VMEM((2, group, HEAD), BF16), pltpu.VMEM((2, HEAD + 8, group), BF16),
                pltpu.VMEM((16, PIECE, d), BF16), pltpu.VMEM((12, PIECE, d), BF16), pltpu.VMEM((PIECE, d), F32),
                pltpu.VMEM((2, PIECE, 4 * HEAD), BF16), pltpu.VMEM((8, 2 * PIECE), F32), pltpu.VMEM((4, HEAD + 8, 2 * PIECE), F32),
                dma((5,)), dma((16,)), dma((16,)), dma((16,)), dma((16,)), dma((16,)), dma((16,)), dma((16,)), dma((16,)),
            ],
            compiler_params=pltpu.CompilerParams(collective_id=0, has_side_effects=True, vmem_limit_bytes=63 * 2**20),
        )(x, gain.reshape(1, d), wq, wk, wv, wo, jnp.asarray(coarse), jnp.asarray(fine))

    tokens, columns = P(("dp", "tp"), None), P(None, "tp")
    return jax.shard_map(
        step,
        mesh=mesh,
        in_specs=(tokens, P(None), columns, columns, columns, P("tp", None)),
        out_specs=tokens,
        check_vma=False,
    )
```

```python
import functools

import jax
import jax.numpy as jnp
import numpy as np
from jax import lax
from jax.experimental import pallas as pl
from jax.experimental.pallas import tpu as pltpu
from jax.sharding import PartitionSpec as P

HEAD = 128
THETA = 10000
NEG = -1e30
HIDDEN = 2 * NEG
LOG2E = 1.4426950408889634
E = HEAD**-0.5 * LOG2E
UNIT = 128
PIECE = 128
BK = 512
F32, BF16 = jnp.float32, jnp.bfloat16

ORDER = [(1, 1, 0), (1, 1, 2), (1, 0, 0), (0, 1, 2), (1, 1, 1), (1, 1, 3), (1, 0, 1), (0, 1, 3),
         (1, 0, 2), (0, 1, 0), (1, 0, 3), (0, 1, 1), (0, 0, 2), (0, 0, 0), (0, 0, 3), (0, 0, 1)]
LANDING = [(0, 0, core, quarter) for core in range(2) for quarter in (0, 2, 1, 3)]
for _qx, _qy in ((2, 0), (3, 1), (0, 2), (1, 3)):
    LANDING += [(1, 0, 0, _qx), (0, 1, 0, _qy), (1, 0, 1, _qx), (0, 1, 1, _qy)]
for _q in range(2):
    LANDING += [(1, 1, core, quarter) for core in range(2) for quarter in (_q, _q + 2)]


def _pick(i, table):
    out = jnp.int32(0)
    for n, value in enumerate(table):
        if value:
            out = out + jnp.where(i == n, jnp.int32(value), jnp.int32(0))
    return out


def _flip(bit, by):
    return bit + by - 2 * bit * by


def _dot(a, b, ca=1, cb=0):
    return lax.dot_general(a, b, (((ca,), (cb,)), ((), ())), preferred_element_type=F32)


def _kernel(x_hbm, gain_ref, wq_hbm, wk_hbm, wv_hbm, wo_hbm, coarse_ref, fine_ref, out_ref,
            x_s, wq_s, wk_s, wv_s, wo_s, xg, q_s, k_s, v_s, near_s, far_s, mine_s, o_s, top_s, most_s, mix_s, sa_s, sb_s,
            load_sem, got_sem, core_sem, xs_sem, ys_sem, near_send, near_got, far_send, far_got):
    me = lax.axis_index("tp")
    mx, my, mc = me // 4, (me // 2) % 2, me % 2
    partner, nx, ny = me + 1 - 2 * mc, me + 4 - 8 * mx, me + 2 - 4 * my

    loads = [pltpu.make_async_copy(a, b, load_sem.at[n])
             for n, (a, b) in enumerate([(x_hbm, x_s), (wq_hbm, wq_s), (wk_hbm, wk_s), (wv_hbm, wv_s), (wo_hbm, wo_s)])]
    for load in loads:
        load.start()
    barrier = pltpu.get_barrier_semaphore()
    for other in (partner, nx, ny):
        pl.semaphore_signal(barrier, inc=1, device_id={"tp": other}, device_id_type=pl.DeviceIdType.MESH)
    pl.semaphore_wait(barrier, 3)
    loads[0].wait()

    def slot(i, rows):
        return xg.at[pl.ds(pl.multiple_of(i * rows, rows), rows), :]

    def remote(src, dst, send, recv, to):
        return pltpu.make_async_remote_copy(src_ref=src, dst_ref=dst, send_sem=send, recv_sem=recv, device_id={"tp": to},
                                            device_id_type=pl.DeviceIdType.MESH)

    def block_to(u, v, sems, to):
        return remote(slot(u, UNIT), slot(v, UNIT), sems.at[u], got_sem.at[v], to)

    gain = gain_ref[...].astype(F32)

    def norm(i, carry):
        at = pl.ds(pl.multiple_of(i * 32, 32), 32)
        wide = x_s[at, :].astype(F32)
        scale = lax.rsqrt(jnp.mean(wide * wide, -1, keepdims=True) + 1e-6)
        xg[at, :] = (wide * scale * gain).astype(BF16)
        return carry

    def send(q, *which):
        for sems, other, by in which:
            block_to(q, q + by, sems, other).start()

    to_core, to_x, to_y = (core_sem, partner, 4), (xs_sem, nx, 16), (ys_sem, ny, 8)
    per = UNIT // 32
    for q in (0, 2, 1, 3):
        lax.fori_loop(q * per, (q + 1) * per, norm, 0)
        if q == 0:
            send(0, to_y, to_core)
        elif q == 2:
            send(2, to_x, to_core)
        elif q == 1:
            send(1, to_y, to_core)
        else:
            send(3, to_x, to_core)
            send(0, to_x)
            send(1, to_x)
            send(2, to_y)
            send(3, to_y)
    for i in range(2):
        v_s[i, HEAD:, :] = jnp.ones((8, v_s.shape[2]), BF16)
    for load in loads[1:]:
        load.wait()

    sign = jnp.where(lax.broadcasted_iota(jnp.int32, (1, HEAD), 1) < HEAD // 2, -1.0, 1.0).astype(F32)

    def landed(n, carry):
        bx, by, bc, quarter = (_pick(n, [row[k] for row in LANDING]) for k in range(4))
        u = 16 * bx + 8 * by + 4 * bc + quarter

        @pl.when(bx + by + bc > 0)
        def _():
            block_to(u, u, core_sem, partner).wait_recv()

        @pl.when((bc == 0) & (bx + by > 0))
        def _():
            block_to(u, u + 4, core_sem, partner).start()

        @pl.when((bc == 0) & (by == 1) & (bx == 0) & (quarter < 2))
        def _():
            block_to(u, 24 + quarter, xs_sem, nx).start()

        @pl.when((bc == 0) & (by == 0) & (bx == 1) & (quarter >= 2))
        def _():
            block_to(u, 24 + quarter, ys_sem, ny).start()

        place = (4 * _flip(mx, bx) + 2 * _flip(my, by) + _flip(mc, bc)) * 4 + quarter
        rows = pl.ds(pl.multiple_of(place * UNIT, UNIT), UNIT)
        base = coarse_ref[pl.ds(place, 1), :]
        cos_a, sin_a = base[:, :HEAD], base[:, HEAD:]
        cos_b, sin_b = fine_ref[:, :HEAD], fine_ref[:, HEAD:]
        cos = cos_a * cos_b - sin_a * sin_b
        sin = (sin_a * cos_b + cos_a * sin_b) * sign

        def turned(t):
            t = t.astype(BF16).astype(F32)
            return (t * cos + pltpu.roll(t, HEAD // 2, 1) * sin).astype(BF16)

        a = slot(u, UNIT)
        q = _dot(a[...], wq_s[...])
        for i in range(4):
            q_s[i, rows, :] = turned(q[:, i * HEAD : (i + 1) * HEAD])
        k = _dot(a[...], wk_s[...])
        for i in range(2):
            k_s[i, rows, :] = turned(k[:, i * HEAD : (i + 1) * HEAD])
        v = _dot(a[...], wv_s[...])
        for i in range(2):
            v_s[i, :HEAD, rows] = v[:, i * HEAD : (i + 1) * HEAD].T.astype(BF16)
        return carry

    lax.fori_loop(0, 32, landed, 0)
    for r in (0, 8, 16, 24):
        for q in range(4):
            block_to(r + q, r + q + 4, core_sem, partner).wait_send()
    for u in (0, 1, 2, 3, 8, 9):
        block_to(u, u, xs_sem, nx).wait_send()
    for u in (0, 1, 2, 3, 18, 19):
        block_to(u, u, ys_sem, ny).wait_send()

    strips = [(i, g) for g in range(2) for i in range(2)]
    strip_of = {s: n for n, s in enumerate(strips)}

    def which(t):
        return tuple(_pick(t, [row[k] for row in ORDER]) for k in range(3))

    bufs = (sa_s, sb_s)

    def score(first, j, n, buf):
        i, g = strips[n]
        keys = pl.ds(pl.multiple_of(j * BK, BK), BK)
        rows = pl.ds(pl.multiple_of(first + g * 512, PIECE), PIECE)
        s = _dot(k_s[i, keys, :], q_s[2 * i : 2 * i + 2, rows, :].reshape(2 * PIECE, HEAD), 1, 1)
        bufs[buf][n] = s
        most_s[4 * buf + n : 4 * buf + n + 1, :] = s.max(axis=0, keepdims=True)

    def absorb(j, n, buf, p, masked):
        i, g = strips[n]
        keys = pl.ds(pl.multiple_of(j * BK, BK), BK)
        s = bufs[buf][n]
        if masked:
            gap = (lax.broadcasted_iota(jnp.int32, (BK, 2 * PIECE), 1) % PIECE) - lax.broadcasted_iota(jnp.int32, (BK, 2 * PIECE), 0)
            s = jnp.where(gap + p * PIECE >= 0, s, HIDDEN)
            most = s.max(axis=0, keepdims=True)
        else:
            most = most_s[4 * buf + n : 4 * buf + n + 1, :]
        old = top_s[n : n + 1, :]
        top = jnp.maximum(old, most)
        top_s[n : n + 1, :] = top
        w = jnp.exp2((s - top) * E).astype(BF16)
        mix_s[n] = mix_s[n] * jnp.exp2((old - top) * E) + _dot(v_s[i, :, keys], w)

    def attend(t):
        bx, by, p = which(t)
        chip = 2 * _flip(mx, bx) + _flip(my, by)
        first = chip * 1024 + p * PIECE
        top_s[...] = jnp.full(top_s.shape, NEG, F32)
        mix_s[...] = jnp.zeros(mix_s.shape, F32)
        for n in range(4):
            score(first, 0, n, 0)

        def two(c, carry):
            for buf in range(2):
                for n in range(4):
                    score(first, 2 * c + buf + 1, n, 1 - buf)
                    absorb(2 * c + buf, n, buf, p, False)
            return carry

        lax.fori_loop(0, chip, two, 0)
        for n in (2, 3):
            score(first, 2 * chip + 1, n, 1)
        for n in range(4):
            absorb(2 * chip, n, 0, p, n < 2)
        for n in (2, 3):
            absorb(2 * chip + 1, n, 1, p, True)
        for n, (i, g) in enumerate(strips):
            o = (mix_s[n, :HEAD, :] * (1 / mix_s[n, HEAD : HEAD + 1, :])).T.astype(BF16)
            for m in range(2):
                o_s[g, :, (2 * i + m) * HEAD : (2 * i + m + 1) * HEAD] = o[m * PIECE : (m + 1) * PIECE, :]

    def near(t):
        return remote(slot(16 + t, PIECE), near_s.at[t], near_send.at[t], near_got.at[t], partner)

    def far(t, to_slot, to):
        return remote(slot(t, PIECE), far_s.at[to_slot], far_send.at[t], far_got.at[to_slot], to)

    def project(t):
        for n in range(0, 2048, 512):
            slot(16 + t, PIECE)[:, n : n + 512] = _dot(o_s[1 - mc], wo_s[:, n : n + 512]).astype(BF16)
        near(t).start()
        for n in range(0, 2048, 512):
            mine_s[jnp.maximum(t - 11, 0), :, n : n + 512] = _dot(o_s[mc], wo_s[:, n : n + 512])

    def tiles(body):
        def step(i, carry):
            body(pl.ds(pl.multiple_of(i * 32, 32), 32), i * 32)
            return carry

        lax.fori_loop(0, PIECE // 32, step, 0)

    def finish(t):
        bx, by, p = which(t)
        low = p < 2
        near(t).wait_recv()
        summed = ((by == 0) & jnp.logical_not(low)) | ((bx == 0) & low)

        @pl.when(summed)
        def _():
            far(0, p, nx).wait_recv()

            def body(at, i):
                to = pl.ds(pl.multiple_of(t * PIECE + i, 32), 32)
                xg[to, :] = (mine_s[0, at, :] + near_s[t, at, :].astype(F32) + far_s[p, at, :].astype(F32)).astype(BF16)

            tiles(body)

        @pl.when(jnp.logical_not(summed))
        def _():
            def body(at, i):
                to = pl.ds(pl.multiple_of(t * PIECE + i, 32), 32)
                xg[to, :] = (mine_s[0, at, :] + near_s[t, at, :].astype(F32)).astype(BF16)

            tiles(body)

        to_slot = p + 4 * bx * (1 - by) + 8 * by * (1 - bx)
        along_x = (by == 0) | ((bx == 1) & low)

        @pl.when(along_x)
        def _():
            far(t, to_slot, nx).start()

        @pl.when(jnp.logical_not(along_x))
        def _():
            far(t, to_slot, ny).start()

    def conclude(t, carry):
        p = which(t)[2]
        near(t).wait_recv()
        far(0, 4 + p, nx).wait_recv()
        far(0, 8 + p, ny).wait_recv()

        def body(at, i):
            to = pl.ds(pl.multiple_of(p * PIECE + i, 32), 32)
            total = mine_s[t - 11, at, :] + near_s[t, at, :].astype(F32)
            total = total + far_s[4 + p, at, :].astype(F32) + far_s[8 + p, at, :].astype(F32)
            out_ref[to, :] = (x_s[to, :].astype(F32) + total).astype(BF16)

        tiles(body)
        return carry

    def piece(t, carry):
        early = (t == 1) | (t == 2)

        @pl.when(early)
        def _():
            finish(t - 1)

        attend(t)

        @pl.when(jnp.logical_not(early) & (t > 0) & (t <= 12))
        def _():
            finish(t - 1)

        project(t)
        return carry

    lax.fori_loop(0, 16, piece, 0)
    lax.fori_loop(12, 16, conclude, 0)

    def sent(t, carry):
        near(t).wait_send()

        @pl.when(t < 12)
        def _():
            far(t, 0, nx).wait_send()

        return carry

    lax.fori_loop(0, 16, sent, 0)


def tables():
    half = HEAD // 2
    rate = np.concatenate([float(THETA) ** (-np.arange(half) / half)] * 2)
    a = np.arange(32)[:, None] * UNIT * rate
    b = np.arange(UNIT)[:, None] * rate
    both = lambda t: np.concatenate([np.cos(t), np.sin(t)], 1).astype(np.float32)
    return both(a), both(b)


def solution(mesh):
    def step(x, gain, wq, wk, wv, wo):
        rows, d = x.shape
        group = rows * 8
        coarse, fine = tables()
        hbm, vmem = pl.BlockSpec(memory_space=pl.ANY), pl.BlockSpec(memory_space=pltpu.VMEM)
        dma = pltpu.SemaphoreType.DMA
        return pl.pallas_call(
            _kernel,
            out_shape=jax.ShapeDtypeStruct((rows, d), BF16),
            in_specs=[hbm, vmem, hbm, hbm, hbm, hbm, vmem, vmem],
            out_specs=vmem,
            scratch_shapes=[
                pltpu.VMEM(x.shape, BF16), pltpu.VMEM(wq.shape, BF16), pltpu.VMEM(wk.shape, BF16), pltpu.VMEM(wv.shape, BF16),
                pltpu.VMEM(wo.shape, BF16),
                pltpu.VMEM((group, d), BF16),
                pltpu.VMEM((4, group, HEAD), BF16), pltpu.VMEM((2, group, HEAD), BF16), pltpu.VMEM((2, HEAD + 8, group), BF16),
                pltpu.VMEM((16, PIECE, d), BF16), pltpu.VMEM((12, PIECE, d), BF16), pltpu.VMEM((5, PIECE, d), F32),
                pltpu.VMEM((2, PIECE, 4 * HEAD), BF16), pltpu.VMEM((8, 2 * PIECE), F32), pltpu.VMEM((8, 2 * PIECE), F32), pltpu.VMEM((4, HEAD + 8, 2 * PIECE), F32),
                pltpu.VMEM((4, BK, 2 * PIECE), F32), pltpu.VMEM((4, BK, 2 * PIECE), F32),
                dma((5,)), dma((32,)), dma((32,)), dma((32,)), dma((32,)), dma((16,)), dma((16,)), dma((16,)), dma((16,)),
            ],
            compiler_params=pltpu.CompilerParams(collective_id=0, has_side_effects=True, vmem_limit_bytes=63 * 2**20),
        )(x, gain.reshape(1, d), wq, wk, wv, wo, jnp.asarray(coarse), jnp.asarray(fine))

    tokens, columns = P(("dp", "tp"), None), P(None, "tp")
    return jax.shard_map(
        step,
        mesh=mesh,
        in_specs=(tokens, P(None), columns, columns, columns, P("tp", None)),
        out_specs=tokens,
        check_vma=False,
    )
```

```python
import functools

import jax
import jax.numpy as jnp
import numpy as np
from jax import lax
from jax.experimental import pallas as pl
from jax.experimental.pallas import tpu as pltpu
from jax.sharding import PartitionSpec as P

HEAD = 128
THETA = 10000
NEG = -1e30
HIDDEN = 2 * NEG
LOG2E = 1.4426950408889634
E = HEAD**-0.5 * LOG2E
UNIT = 128
PIECE = 128
BK = 512
F32, BF16 = jnp.float32, jnp.bfloat16

OWN, Y, X, D = 0, 4, 8, 12
LAST = [OWN + 2, OWN, OWN + 3, OWN + 1]
ORDER = [
    [Y + 2, X, Y + 3, X + 1, D, D + 2, D + 1, D + 3, Y, X + 2, Y + 1, X + 3] + LAST,
    [Y + 2, Y + 3, D, X, D + 1, X + 1, D + 2, D + 3, X + 2, Y, X + 3, Y + 1] + LAST,
    [X, X + 1, D + 2, Y + 2, D + 3, Y + 3, D, D + 1, Y, X + 2, Y + 1, X + 3] + LAST,
    [D, D + 2, D + 1, D + 3, X, Y + 2, X + 1, Y + 3, X + 2, Y, X + 3, Y + 1] + LAST,
]
EARLY = [4, 2, 2, 0]
LANDING = [4 * core + quarter for core in range(2) for quarter in (0, 2, 1, 3)]
for _qx, _qy in ((2, 0), (3, 1), (0, 2), (1, 3)):
    LANDING += [16 + _qx, 8 + _qy, 20 + _qx, 12 + _qy]
for _q in range(2):
    LANDING += [24 + _q, 26 + _q, 28 + _q, 30 + _q]


def _choose(i, values):
    out = jnp.int32(values[-1])
    for n, value in enumerate(values[:-1]):
        out = jnp.where(i == n, jnp.int32(value), out)
    return out


def _packed(row, bits):
    per = 32 // bits
    words = [sum(v << (bits * n) for n, v in enumerate(row[at : at + per])) for at in range(0, len(row), per)]
    return [w - 2**32 if w >= 2**31 else w for w in words]


def _unpacked(i, words, bits):
    per = 32 // bits
    return (_choose(i // per, words) >> (bits * (i % per))) & (2**bits - 1)


def _flip(bit, by):
    return bit + by - 2 * bit * by


def _dot(a, b, ca=1, cb=0):
    return lax.dot_general(a, b, (((ca,), (cb,)), ((), ())), preferred_element_type=F32)


def _kernel(x_hbm, gain_ref, wq_hbm, wk_hbm, wv_hbm, wo_hbm, coarse_ref, fine_ref, out_ref,
            x_s, wq_s, wk_s, wv_s, wo_s, xg, q_s, k_s, v_s, near_s, far_s, mine_s, o_s, top_s, most_s, mix_s, sa_s, sb_s,
            load_sem, got_sem, core_sem, xs_sem, ys_sem, near_send, near_got, far_send, far_got):
    me = lax.axis_index("tp")
    mx, my, mc = me // 4, (me // 2) % 2, me % 2
    partner, nx, ny = me + 1 - 2 * mc, me + 4 - 8 * mx, me + 2 - 4 * my

    loads = [pltpu.make_async_copy(a, b, load_sem.at[n])
             for n, (a, b) in enumerate([(x_hbm, x_s), (wq_hbm, wq_s), (wk_hbm, wk_s), (wv_hbm, wv_s), (wo_hbm, wo_s)])]
    for load in loads:
        load.start()
    barrier = pltpu.get_barrier_semaphore()
    for other in (partner, nx, ny):
        pl.semaphore_signal(barrier, inc=1, device_id={"tp": other}, device_id_type=pl.DeviceIdType.MESH)
    pl.semaphore_wait(barrier, 3)
    loads[0].wait()

    def slot(i, rows):
        return xg.at[pl.ds(pl.multiple_of(i * rows, rows), rows), :]

    def remote(src, dst, send, recv, to):
        return pltpu.make_async_remote_copy(src_ref=src, dst_ref=dst, send_sem=send, recv_sem=recv, device_id={"tp": to},
                                            device_id_type=pl.DeviceIdType.MESH)

    def block_to(u, v, sems, to):
        return remote(slot(u, UNIT), slot(v, UNIT), sems.at[u], got_sem.at[v], to)

    gain = gain_ref[...].reshape(1, -1).astype(F32)

    def norm(i, carry):
        at = pl.ds(pl.multiple_of(i * 32, 32), 32)
        wide = x_s[at, :].astype(F32)
        scale = lax.rsqrt(jnp.mean(wide * wide, -1, keepdims=True) + 1e-6)
        xg[at, :] = (wide * scale * gain).astype(BF16)
        return carry

    def send(q, *which):
        for sems, other, by in which:
            block_to(q, q + by, sems, other).start()

    to_core, to_x, to_y = (core_sem, partner, 4), (xs_sem, nx, 16), (ys_sem, ny, 8)
    per = UNIT // 32
    for q in (0, 2, 1, 3):
        lax.fori_loop(q * per, (q + 1) * per, norm, 0)
        if q == 0:
            send(0, to_y, to_core)
        elif q == 2:
            send(2, to_x, to_core)
        elif q == 1:
            send(1, to_y, to_core)
        else:
            send(3, to_x, to_core)
            send(0, to_x)
            send(1, to_x)
            send(2, to_y)
            send(3, to_y)
    for i in range(2):
        v_s[i, HEAD:, :] = jnp.ones((8, v_s.shape[2]), BF16)
    for load in loads[1:]:
        load.wait()

    sign = jnp.where(lax.broadcasted_iota(jnp.int32, (1, HEAD), 1) < HEAD // 2, -1.0, 1.0).astype(F32)

    chip = 2 * mx + my
    early = _choose(chip, EARLY)
    strips = [(i, g) for g in range(2) for i in range(2)]
    strip_of = {s: n for n, s in enumerate(strips)}

    orders = [_packed(row, 4) for row in ORDER]
    order = [_choose(chip, [row[n] for row in orders]) for n in range(2)]

    def which(t):
        piece = (jnp.where(t < 8, order[0], order[1]) >> (4 * (t % 8))) & 15
        return piece // 8, (piece // 4) % 2, piece % 4

    bufs = (sa_s, sb_s)

    def score(first, j, n, buf):
        i, g = strips[n]
        keys = pl.ds(pl.multiple_of(j * BK, BK), BK)
        rows = pl.ds(pl.multiple_of(first + g * 512, PIECE), PIECE)
        s = _dot(k_s[i, keys, :], q_s[2 * i : 2 * i + 2, rows, :].reshape(2 * PIECE, HEAD), 1, 1)
        bufs[buf][n] = s
        most_s[4 * buf + n : 4 * buf + n + 1, :] = s.max(axis=0, keepdims=True)

    def absorb(j, n, buf, p, masked):
        i, g = strips[n]
        keys = pl.ds(pl.multiple_of(j * BK, BK), BK)
        s = bufs[buf][n]
        if masked:
            gap = (lax.broadcasted_iota(jnp.int32, (BK, 2 * PIECE), 1) % PIECE) - lax.broadcasted_iota(jnp.int32, (BK, 2 * PIECE), 0)
            s = jnp.where(gap + p * PIECE >= 0, s, HIDDEN)
            most = s.max(axis=0, keepdims=True)
        else:
            most = most_s[4 * buf + n : 4 * buf + n + 1, :]
        old = top_s[n : n + 1, :]
        top = jnp.maximum(old, most)
        top_s[n : n + 1, :] = top
        w = jnp.exp2((s - top) * E).astype(BF16)
        mix_s[n] = mix_s[n] * jnp.exp2((old - top) * E) + _dot(v_s[i, :, keys], w)

    def attend(t):
        bx, by, p = which(t)
        there = 2 * _flip(mx, bx) + _flip(my, by)
        first = there * 1024 + p * PIECE
        top_s[...] = jnp.full(top_s.shape, NEG, F32)
        mix_s[...] = jnp.zeros(mix_s.shape, F32)
        for n in range(4):
            score(first, 0, n, 0)

        def two(c, carry):
            for buf in range(2):
                for n in range(4):
                    score(first, 2 * c + buf + 1, n, 1 - buf)
                    absorb(2 * c + buf, n, buf, p, False)
            return carry

        lax.fori_loop(0, there, two, 0)
        for n in (2, 3):
            score(first, 2 * there + 1, n, 1)
        for n in range(4):
            absorb(2 * there, n, 0, p, n < 2)
        for n in (2, 3):
            absorb(2 * there + 1, n, 1, p, True)
        for n, (i, g) in enumerate(strips):
            o = (mix_s[n, :HEAD, :] * (1 / mix_s[n, HEAD : HEAD + 1, :])).T.astype(BF16)
            for m in range(2):
                o_s[g, :, (2 * i + m) * HEAD : (2 * i + m + 1) * HEAD] = o[m * PIECE : (m + 1) * PIECE, :]

    def near_slot(t):
        return jnp.where(t < 4, 4 + t, 12 + t)

    def far_slot(t):
        return jnp.where(t < 4, 12 + t, jnp.where(t < 8, t - 4, t))

    def near(t):
        return remote(slot(near_slot(t), PIECE), near_s.at[t], near_send.at[t], near_got.at[t], partner)

    def far(t, to_slot, to):
        return remote(slot(far_slot(t), PIECE), far_s.at[to_slot], far_send.at[t], far_got.at[to_slot], to)

    def project(t):
        for n in range(0, 2048, 512):
            slot(near_slot(t), PIECE)[:, n : n + 512] = _dot(o_s[1 - mc], wo_s[:, n : n + 512]).astype(BF16)
        near(t).start()
        for n in range(0, 2048, 512):
            mine_s[jnp.maximum(t - 11, 0), :, n : n + 512] = _dot(o_s[mc], wo_s[:, n : n + 512])

    def tiles(body):
        def step(i, carry):
            body(pl.ds(pl.multiple_of(i * 32, 32), 32), i * 32)
            return carry

        lax.fori_loop(0, PIECE // 32, step, 0)

    def finish(t):
        bx, by, p = which(t)
        low = p < 2
        near(t).wait_recv()
        summed = ((by == 0) & jnp.logical_not(low)) | ((bx == 0) & low)

        @pl.when(summed)
        def _():
            far(0, p, nx).wait_recv()

            def body(at, i):
                to = pl.ds(pl.multiple_of(far_slot(t) * PIECE + i, 32), 32)
                xg[to, :] = (mine_s[0, at, :] + near_s[t, at, :].astype(F32) + far_s[p, at, :].astype(F32)).astype(BF16)

            tiles(body)

        @pl.when(jnp.logical_not(summed))
        def _():
            def body(at, i):
                to = pl.ds(pl.multiple_of(far_slot(t) * PIECE + i, 32), 32)
                xg[to, :] = (mine_s[0, at, :] + near_s[t, at, :].astype(F32)).astype(BF16)

            tiles(body)

        to_slot = p + 4 * bx * (1 - by) + 8 * by * (1 - bx)
        along_x = (by == 0) | ((bx == 1) & low)

        @pl.when(along_x)
        def _():
            far(t, to_slot, nx).start()

        @pl.when(jnp.logical_not(along_x))
        def _():
            far(t, to_slot, ny).start()

    def conclude(t, carry):
        p = which(t)[2]
        near(t).wait_recv()
        far(0, 4 + p, nx).wait_recv()
        far(0, 8 + p, ny).wait_recv()

        def body(at, i):
            to = pl.ds(pl.multiple_of(p * PIECE + i, 32), 32)
            total = mine_s[t - 11, at, :] + near_s[t, at, :].astype(F32)
            total = total + far_s[4 + p, at, :].astype(F32) + far_s[8 + p, at, :].astype(F32)
            out_ref[to, :] = (x_s[to, :].astype(F32) + total).astype(BF16)

        tiles(body)
        return carry

    def ahead_of_time(t, carry):
        attend(t)
        project(t)
        finish(t)
        return carry

    def landed(n, carry):
        ahead = jnp.minimum(early, 2)
        first = jnp.where(n == 28, ahead, 0)
        lax.fori_loop(first, jnp.where(n == 24, ahead, jnp.where(n == 28, early, 0)), ahead_of_time, 0)
        u = _unpacked(n, _packed(LANDING, 8), 8)
        bx, by, bc, quarter = u // 16, (u // 8) % 2, (u // 4) % 2, u % 4

        @pl.when(bx + by + bc > 0)
        def _():
            block_to(u, u, core_sem, partner).wait_recv()

        @pl.when((bc == 0) & (bx + by > 0))
        def _():
            block_to(u, u + 4, core_sem, partner).start()

        @pl.when((bc == 0) & (by == 1) & (bx == 0) & (quarter < 2))
        def _():
            block_to(u, 24 + quarter, xs_sem, nx).start()

        @pl.when((bc == 0) & (by == 0) & (bx == 1) & (quarter >= 2))
        def _():
            block_to(u, 24 + quarter, ys_sem, ny).start()

        place = (4 * _flip(mx, bx) + 2 * _flip(my, by) + _flip(mc, bc)) * 4 + quarter
        rows = pl.ds(pl.multiple_of(place * UNIT, UNIT), UNIT)
        base = coarse_ref[pl.ds(place, 1), :]
        cos_a, sin_a = base[:, :HEAD], base[:, HEAD:]
        cos_b, sin_b = fine_ref[:, :HEAD], fine_ref[:, HEAD:]
        cos = cos_a * cos_b - sin_a * sin_b
        sin = (sin_a * cos_b + cos_a * sin_b) * sign

        def turned(t):
            t = t.astype(BF16).astype(F32)
            return (t * cos + pltpu.roll(t, HEAD // 2, 1) * sin).astype(BF16)

        a = slot(u, UNIT)
        q = _dot(a[...], wq_s[...])
        for i in range(4):
            q_s[i, rows, :] = turned(q[:, i * HEAD : (i + 1) * HEAD])
        k = _dot(a[...], wk_s[...])
        for i in range(2):
            k_s[i, rows, :] = turned(k[:, i * HEAD : (i + 1) * HEAD])
        v = _dot(a[...], wv_s[...])
        for i in range(2):
            v_s[i, :HEAD, rows] = v[:, i * HEAD : (i + 1) * HEAD].T.astype(BF16)
        return carry

    lax.fori_loop(0, 32, landed, 0)
    for r in (0, 8, 16, 24):
        for q in range(4):
            block_to(r + q, r + q + 4, core_sem, partner).wait_send()
    for u in (0, 1, 2, 3, 8, 9):
        block_to(u, u, xs_sem, nx).wait_send()
    for u in (0, 1, 2, 3, 18, 19):
        block_to(u, u, ys_sem, ny).wait_send()

    def piece(t, carry):
        soon = ((early == 2) & (t == 3)) | ((early == 0) & (t == 2))

        @pl.when(soon)
        def _():
            finish(t - 1)

        attend(t)

        @pl.when(jnp.logical_not(soon) & (t > early) & (t <= 12))
        def _():
            finish(t - 1)

        project(t)
        return carry

    lax.fori_loop(early, 16, piece, 0)
    lax.fori_loop(12, 16, conclude, 0)

    def sent(t, carry):
        near(t).wait_send()

        @pl.when(t < 12)
        def _():
            far(t, 0, nx).wait_send()

        return carry

    lax.fori_loop(0, 16, sent, 0)


def tables():
    half = HEAD // 2
    rate = np.concatenate([float(THETA) ** (-np.arange(half) / half)] * 2)
    a = np.arange(32)[:, None] * UNIT * rate
    b = np.arange(UNIT)[:, None] * rate
    both = lambda t: np.concatenate([np.cos(t), np.sin(t)], 1).astype(np.float32)
    return both(a), both(b)


def solution(mesh):
    def step(x, gain, wq, wk, wv, wo):
        rows, d = x.shape
        group = rows * 8
        coarse, fine = tables()
        hbm, vmem = pl.BlockSpec(memory_space=pl.ANY), pl.BlockSpec(memory_space=pltpu.VMEM)
        dma = pltpu.SemaphoreType.DMA
        return pl.pallas_call(
            _kernel,
            out_shape=jax.ShapeDtypeStruct((rows, d), BF16),
            in_specs=[hbm, vmem, hbm, hbm, hbm, hbm, vmem, vmem],
            out_specs=vmem,
            scratch_shapes=[
                pltpu.VMEM(x.shape, BF16), pltpu.VMEM(wq.shape, BF16), pltpu.VMEM(wk.shape, BF16), pltpu.VMEM(wv.shape, BF16),
                pltpu.VMEM(wo.shape, BF16),
                pltpu.VMEM((group, d), BF16),
                pltpu.VMEM((4, group, HEAD), BF16), pltpu.VMEM((2, group, HEAD), BF16), pltpu.VMEM((2, HEAD + 8, group), BF16),
                pltpu.VMEM((16, PIECE, d), BF16), pltpu.VMEM((12, PIECE, d), BF16), pltpu.VMEM((5, PIECE, d), F32),
                pltpu.VMEM((2, PIECE, 4 * HEAD), BF16), pltpu.VMEM((8, 2 * PIECE), F32), pltpu.VMEM((8, 2 * PIECE), F32), pltpu.VMEM((4, HEAD + 8, 2 * PIECE), F32),
                pltpu.VMEM((4, BK, 2 * PIECE), F32), pltpu.VMEM((4, BK, 2 * PIECE), F32),
                dma((5,)), dma((32,)), dma((32,)), dma((32,)), dma((32,)), dma((16,)), dma((16,)), dma((16,)), dma((16,)),
            ],
            compiler_params=pltpu.CompilerParams(collective_id=0, has_side_effects=True, vmem_limit_bytes=63 * 2**20),
        )(x, gain, wq, wk, wv, wo, jnp.asarray(coarse), jnp.asarray(fine))

    tokens, columns = P(("dp", "tp"), None), P(None, "tp")
    return jax.shard_map(
        step,
        mesh=mesh,
        in_specs=(tokens, P(None), columns, columns, columns, P("tp", None)),
        out_specs=tokens,
        check_vma=False,
    )
```

```python
import functools

import jax
import jax.numpy as jnp
import numpy as np
from jax import lax
from jax.experimental import pallas as pl
from jax.experimental.pallas import tpu as pltpu
from jax.sharding import PartitionSpec as P

HEAD = 128
THETA = 10000
NEG = -1e30
HIDDEN = 2 * NEG
LOG2E = 1.4426950408889634
E = HEAD**-0.5 * LOG2E
UNIT = 128
PIECE = 128
BK = 512
F32, BF16 = jnp.float32, jnp.bfloat16

OWN, Y, X, D = 0, 4, 8, 12
LAST = [OWN + 2, OWN, OWN + 3, OWN + 1]
ORDER = [
    [Y + 2, X, Y + 3, X + 1, D, D + 2, D + 1, D + 3, Y, X + 2, Y + 1, X + 3] + LAST,
    [Y + 2, Y + 3, D, X, D + 2, D + 1, D + 3, X + 1, X + 2, Y, X + 3, Y + 1] + LAST,
    [X, X + 1, D + 2, Y + 2, D, D + 3, D + 1, Y + 3, Y, X + 2, Y + 1, X + 3] + LAST,
    [D, D + 2, D + 1, D + 3, X, Y + 2, X + 1, Y + 3, X + 2, Y, X + 3, Y + 1] + LAST,
]
EARLY = [4, 2, 2, 4]
_OWNED = [4 * core + quarter for core in range(2) for quarter in (0, 2, 1, 3)]
_FIRST = [u for a, b in ((18, 8), (19, 9)) for u in (a, b, a + 4, b + 4)]
_SECOND = [u for a, b in ((16, 10), (17, 11)) for u in (a, b, a + 4, b + 4)]
_ACROSS = [u for a, b in ((24, 26), (25, 27)) for u in (a, b, a + 4, b + 4)]
LANDING = [_OWNED + _FIRST + _SECOND + _ACROSS, _OWNED + _FIRST + _ACROSS + _SECOND]


def _choose(i, values):
    out = jnp.int32(values[-1])
    for n, value in enumerate(values[:-1]):
        out = jnp.where(i == n, jnp.int32(value), out)
    return out


def _packed(row, bits):
    per = 32 // bits
    words = [sum(v << (bits * n) for n, v in enumerate(row[at : at + per])) for at in range(0, len(row), per)]
    return [w - 2**32 if w >= 2**31 else w for w in words]


def _unpacked(i, words, bits):
    per = 32 // bits
    return (_choose(i // per, words) >> (bits * (i % per))) & (2**bits - 1)


def _flip(bit, by):
    return bit + by - 2 * bit * by


def _dot(a, b, ca=1, cb=0):
    return lax.dot_general(a, b, (((ca,), (cb,)), ((), ())), preferred_element_type=F32)


def _kernel(x_hbm, gain_ref, wq_hbm, wk_hbm, wv_hbm, wo_hbm, coarse_ref, fine_ref, out_ref,
            x_s, wq_s, wk_s, wv_s, wo_s, xg, q_s, k_s, v_s, near_s, far_s, mine_s, o_s, top_s, most_s, mix_s, sa_s, sb_s,
            load_sem, got_sem, core_sem, xs_sem, ys_sem, near_send, near_got, far_send, far_got):
    me = lax.axis_index("tp")
    mx, my, mc = me // 4, (me // 2) % 2, me % 2
    partner, nx, ny = me + 1 - 2 * mc, me + 4 - 8 * mx, me + 2 - 4 * my

    loads = [pltpu.make_async_copy(a, b, load_sem.at[n])
             for n, (a, b) in enumerate([(x_hbm, x_s), (wq_hbm, wq_s), (wk_hbm, wk_s), (wv_hbm, wv_s), (wo_hbm, wo_s)])]
    for load in loads:
        load.start()
    barrier = pltpu.get_barrier_semaphore()
    for other in (partner, nx, ny):
        pl.semaphore_signal(barrier, inc=1, device_id={"tp": other}, device_id_type=pl.DeviceIdType.MESH)
    pl.semaphore_wait(barrier, 3)
    loads[0].wait()

    def slot(i, rows):
        return xg.at[pl.ds(pl.multiple_of(i * rows, rows), rows), :]

    def remote(src, dst, send, recv, to):
        return pltpu.make_async_remote_copy(src_ref=src, dst_ref=dst, send_sem=send, recv_sem=recv, device_id={"tp": to},
                                            device_id_type=pl.DeviceIdType.MESH)

    def block_to(u, v, sems, to):
        return remote(slot(u, UNIT), slot(v, UNIT), sems.at[u], got_sem.at[v], to)

    gain = gain_ref[...].reshape(1, -1).astype(F32)

    def norm(i, carry):
        at = pl.ds(pl.multiple_of(i * 32, 32), 32)
        wide = x_s[at, :].astype(F32)
        scale = lax.rsqrt(jnp.mean(wide * wide, -1, keepdims=True) + 1e-6)
        xg[at, :] = (wide * scale * gain).astype(BF16)
        return carry

    chip = 2 * mx + my
    early = _choose(chip, EARLY)

    def send(q, *which):
        for sems, other, by in which:
            block_to(q, q + by, sems, other).start()

    to_core, to_x, to_y = (core_sem, partner, 4), (xs_sem, nx, 16), (ys_sem, ny, 8)
    per = UNIT // 32
    for q in (0, 2, 1, 3):
        lax.fori_loop(q * per, (q + 1) * per, norm, 0)
        if q == 0:
            send(0, to_y, to_core)
        elif q == 2:
            send(2, to_x, to_core)
        elif q == 1:
            send(1, to_y, to_core)
        else:
            send(3, to_x, to_core)

            @pl.when(chip != 1)
            def _():
                send(0, to_x)
                send(1, to_x)

            @pl.when(chip != 2)
            def _():
                send(2, to_y)
                send(3, to_y)
    for i in range(2):
        v_s[i, HEAD:, :] = jnp.ones((8, v_s.shape[2]), BF16)
    for load in loads[1:]:
        load.wait()

    sign = jnp.where(lax.broadcasted_iota(jnp.int32, (1, HEAD), 1) < HEAD // 2, -1.0, 1.0).astype(F32)

    strips = [(i, g) for g in range(2) for i in range(2)]
    strip_of = {s: n for n, s in enumerate(strips)}

    orders = [_packed(row, 4) for row in ORDER]
    order = [_choose(chip, [row[n] for row in orders]) for n in range(2)]

    def which(t):
        piece = (jnp.where(t < 8, order[0], order[1]) >> (4 * (t % 8))) & 15
        return piece // 8, (piece // 4) % 2, piece % 4

    bufs = (sa_s, sb_s)

    def score(first, j, n, buf):
        i, g = strips[n]
        keys = pl.ds(pl.multiple_of(j * BK, BK), BK)
        rows = pl.ds(pl.multiple_of(first + g * 512, PIECE), PIECE)
        s = _dot(k_s[i, keys, :], q_s[2 * i : 2 * i + 2, rows, :].reshape(2 * PIECE, HEAD), 1, 1)
        bufs[buf][n] = s
        most_s[4 * buf + n : 4 * buf + n + 1, :] = s.max(axis=0, keepdims=True)

    def absorb(j, n, buf, p, masked):
        i, g = strips[n]
        keys = pl.ds(pl.multiple_of(j * BK, BK), BK)
        s = bufs[buf][n]
        if masked:
            gap = (lax.broadcasted_iota(jnp.int32, (BK, 2 * PIECE), 1) % PIECE) - lax.broadcasted_iota(jnp.int32, (BK, 2 * PIECE), 0)
            s = jnp.where(gap + p * PIECE >= 0, s, HIDDEN)
            most = s.max(axis=0, keepdims=True)
        else:
            most = most_s[4 * buf + n : 4 * buf + n + 1, :]
        old = top_s[n : n + 1, :]
        top = jnp.maximum(old, most)
        top_s[n : n + 1, :] = top
        w = jnp.exp2((s - top) * E).astype(BF16)
        mix_s[n] = mix_s[n] * jnp.exp2((old - top) * E) + _dot(v_s[i, :, keys], w)

    def attend(t):
        bx, by, p = which(t)
        there = 2 * _flip(mx, bx) + _flip(my, by)
        first = there * 1024 + p * PIECE
        top_s[...] = jnp.full(top_s.shape, NEG, F32)
        mix_s[...] = jnp.zeros(mix_s.shape, F32)
        for n in range(4):
            score(first, 0, n, 0)

        def two(c, carry):
            for buf in range(2):
                for n in range(4):
                    score(first, 2 * c + buf + 1, n, 1 - buf)
                    absorb(2 * c + buf, n, buf, p, False)
            return carry

        lax.fori_loop(0, there, two, 0)
        for n in (2, 3):
            score(first, 2 * there + 1, n, 1)
        for n in range(4):
            absorb(2 * there, n, 0, p, n < 2)
        for n in (2, 3):
            absorb(2 * there + 1, n, 1, p, True)
        for n, (i, g) in enumerate(strips):
            o = (mix_s[n, :HEAD, :] * (1 / mix_s[n, HEAD : HEAD + 1, :])).T.astype(BF16)
            for m in range(2):
                o_s[g, :, (2 * i + m) * HEAD : (2 * i + m + 1) * HEAD] = o[m * PIECE : (m + 1) * PIECE, :]

    def near_slot(t):
        return jnp.where(t < 4, 4 + t, jnp.where(t < 10, 12 + t, 14 + t))

    def far_slot(t):
        return jnp.where(t < 2, 12 + t, jnp.where(t < 4, 20 + t, jnp.where(t < 8, t - 4, t)))

    def near(t):
        return remote(slot(near_slot(t), PIECE), near_s.at[t], near_send.at[t], near_got.at[t], partner)

    def far(t, to_slot, to):
        return remote(slot(far_slot(t), PIECE), far_s.at[to_slot], far_send.at[t], far_got.at[to_slot], to)

    def project(t):
        for n in range(0, 2048, 512):
            slot(near_slot(t), PIECE)[:, n : n + 512] = _dot(o_s[1 - mc], wo_s[:, n : n + 512]).astype(BF16)
        near(t).start()
        for n in range(0, 2048, 512):
            mine_s[jnp.maximum(t - 11, 0), :, n : n + 512] = _dot(o_s[mc], wo_s[:, n : n + 512])

    def tiles(body):
        def step(i, carry):
            body(pl.ds(pl.multiple_of(i * 32, 32), 32), i * 32)
            return carry

        lax.fori_loop(0, PIECE // 32, step, 0)

    def finish(t):
        bx, by, p = which(t)
        low = p < 2
        near(t).wait_recv()
        summed = ((by == 0) & jnp.logical_not(low)) | ((bx == 0) & low)

        @pl.when(summed)
        def _():
            far(0, p, nx).wait_recv()

            def body(at, i):
                to = pl.ds(pl.multiple_of(far_slot(t) * PIECE + i, 32), 32)
                xg[to, :] = (mine_s[0, at, :] + near_s[t, at, :].astype(F32) + far_s[p, at, :].astype(F32)).astype(BF16)

            tiles(body)

        @pl.when(jnp.logical_not(summed))
        def _():
            def body(at, i):
                to = pl.ds(pl.multiple_of(far_slot(t) * PIECE + i, 32), 32)
                xg[to, :] = (mine_s[0, at, :] + near_s[t, at, :].astype(F32)).astype(BF16)

            tiles(body)

        to_slot = p + 4 * bx * (1 - by) + 8 * by * (1 - bx)
        along_x = (by == 0) | ((bx == 1) & low)

        @pl.when(along_x)
        def _():
            far(t, to_slot, nx).start()

        @pl.when(jnp.logical_not(along_x))
        def _():
            far(t, to_slot, ny).start()

    def conclude(t, carry):
        p = which(t)[2]
        near(t).wait_recv()
        far(0, 4 + p, nx).wait_recv()
        far(0, 8 + p, ny).wait_recv()

        def body(at, i):
            to = pl.ds(pl.multiple_of(p * PIECE + i, 32), 32)
            total = mine_s[t - 11, at, :] + near_s[t, at, :].astype(F32)
            total = total + far_s[4 + p, at, :].astype(F32) + far_s[8 + p, at, :].astype(F32)
            out_ref[to, :] = (x_s[to, :].astype(F32) + total).astype(BF16)

        tiles(body)
        return carry

    def ahead_of_time(t, carry):
        attend(t)
        project(t)
        finish(t)
        return carry

    def landed(n, carry):
        ahead = jnp.minimum(early, 2)
        first = jnp.where(n == 28, ahead, 0)
        lax.fori_loop(first, jnp.where(n == 24, ahead, jnp.where(n == 28, early, 0)), ahead_of_time, 0)
        u = jnp.where(chip == 3, *(_unpacked(n, _packed(row, 8), 8) for row in LANDING[::-1]))
        bx, by, bc, quarter = u // 16, (u // 8) % 2, (u // 4) % 2, u % 4

        @pl.when(bx + by + bc > 0)
        def _():
            block_to(u, u, core_sem, partner).wait_recv()

        @pl.when((bc == 0) & (bx + by > 0))
        def _():
            block_to(u, u + 4, core_sem, partner).start()

        @pl.when((bc == 0) & (by == 1) & (bx == 0) & (quarter < 2))
        def _():
            block_to(u, 24 + quarter, xs_sem, nx).start()

            @pl.when((chip == 1) & (quarter == 1))
            def _():
                send(0, to_x)
                send(1, to_x)

        @pl.when((bc == 0) & (by == 0) & (bx == 1) & (quarter >= 2))
        def _():
            block_to(u, 24 + quarter, ys_sem, ny).start()

            @pl.when((chip == 2) & (quarter == 3))
            def _():
                send(2, to_y)
                send(3, to_y)

        place = (4 * _flip(mx, bx) + 2 * _flip(my, by) + _flip(mc, bc)) * 4 + quarter
        rows = pl.ds(pl.multiple_of(place * UNIT, UNIT), UNIT)
        base = coarse_ref[pl.ds(place, 1), :]
        cos_a, sin_a = base[:, :HEAD], base[:, HEAD:]
        cos_b, sin_b = fine_ref[:, :HEAD], fine_ref[:, HEAD:]
        cos = cos_a * cos_b - sin_a * sin_b
        sin = (sin_a * cos_b + cos_a * sin_b) * sign

        def turned(t):
            t = t.astype(BF16).astype(F32)
            return (t * cos + pltpu.roll(t, HEAD // 2, 1) * sin).astype(BF16)

        a = slot(u, UNIT)
        q = _dot(a[...], wq_s[...])
        for i in range(4):
            q_s[i, rows, :] = turned(q[:, i * HEAD : (i + 1) * HEAD])
        k = _dot(a[...], wk_s[...])
        for i in range(2):
            k_s[i, rows, :] = turned(k[:, i * HEAD : (i + 1) * HEAD])
        v = _dot(a[...], wv_s[...])
        for i in range(2):
            v_s[i, :HEAD, rows] = v[:, i * HEAD : (i + 1) * HEAD].T.astype(BF16)
        return carry

    lax.fori_loop(0, 32, landed, 0)
    for r in (0, 8, 16, 24):
        for q in range(4):
            block_to(r + q, r + q + 4, core_sem, partner).wait_send()
    for u in (0, 1, 2, 3, 8, 9):
        block_to(u, u, xs_sem, nx).wait_send()
    for u in (0, 1, 2, 3, 18, 19):
        block_to(u, u, ys_sem, ny).wait_send()

    def piece(t, carry):
        soon = (early == 2) & (t == 3)

        @pl.when(soon)
        def _():
            finish(t - 1)

        attend(t)

        @pl.when(jnp.logical_not(soon) & (t > early) & (t <= 12))
        def _():
            finish(t - 1)

        project(t)
        return carry

    lax.fori_loop(early, 16, piece, 0)
    lax.fori_loop(12, 16, conclude, 0)

    def sent(t, carry):
        near(t).wait_send()

        @pl.when(t < 12)
        def _():
            far(t, 0, nx).wait_send()

        return carry

    lax.fori_loop(0, 16, sent, 0)


def tables():
    half = HEAD // 2
    rate = np.concatenate([float(THETA) ** (-np.arange(half) / half)] * 2)
    a = np.arange(32)[:, None] * UNIT * rate
    b = np.arange(UNIT)[:, None] * rate
    both = lambda t: np.concatenate([np.cos(t), np.sin(t)], 1).astype(np.float32)
    return both(a), both(b)


def solution(mesh):
    def step(x, gain, wq, wk, wv, wo):
        rows, d = x.shape
        group = rows * 8
        coarse, fine = tables()
        hbm, vmem = pl.BlockSpec(memory_space=pl.ANY), pl.BlockSpec(memory_space=pltpu.VMEM)
        dma = pltpu.SemaphoreType.DMA
        return pl.pallas_call(
            _kernel,
            out_shape=pltpu.VMEM((rows, d), BF16),
            in_specs=[hbm, vmem, hbm, hbm, hbm, hbm, vmem, vmem],
            out_specs=vmem,
            scratch_shapes=[
                pltpu.VMEM(x.shape, BF16), pltpu.VMEM(wq.shape, BF16), pltpu.VMEM(wk.shape, BF16), pltpu.VMEM(wv.shape, BF16),
                pltpu.VMEM(wo.shape, BF16),
                pltpu.VMEM((group, d), BF16),
                pltpu.VMEM((4, group, HEAD), BF16), pltpu.VMEM((2, group, HEAD), BF16), pltpu.VMEM((2, HEAD + 8, group), BF16),
                pltpu.VMEM((16, PIECE, d), BF16), pltpu.VMEM((12, PIECE, d), BF16), pltpu.VMEM((5, PIECE, d), F32),
                pltpu.VMEM((2, PIECE, 4 * HEAD), BF16), pltpu.VMEM((8, 2 * PIECE), F32), pltpu.VMEM((8, 2 * PIECE), F32), pltpu.VMEM((4, HEAD + 8, 2 * PIECE), F32),
                pltpu.VMEM((4, BK, 2 * PIECE), F32), pltpu.VMEM((4, BK, 2 * PIECE), F32),
                dma((5,)), dma((32,)), dma((32,)), dma((32,)), dma((32,)), dma((16,)), dma((16,)), dma((16,)), dma((16,)),
            ],
            compiler_params=pltpu.CompilerParams(collective_id=0, has_side_effects=True, vmem_limit_bytes=60 * 2**20),
        )(x, gain, wq, wk, wv, wo, jnp.asarray(coarse), jnp.asarray(fine))

    tokens, columns = P(("dp", "tp"), None), P(None, "tp")
    return jax.shard_map(
        step,
        mesh=mesh,
        in_specs=(tokens, P(None), columns, columns, columns, P("tp", None)),
        out_specs=tokens,
        check_vma=False,
    )
```

```python
import functools

import jax
import jax.numpy as jnp
import numpy as np
from jax import lax
from jax.experimental import pallas as pl
from jax.experimental.pallas import tpu as pltpu
from jax.sharding import PartitionSpec as P

HEAD = 128
THETA = 10000
NEG = -1e30
HIDDEN = 2 * NEG
LOG2E = 1.4426950408889634
E = HEAD**-0.5 * LOG2E
UNIT = 128
PIECE = 128
BK = 512
F32, BF16 = jnp.float32, jnp.bfloat16

OWN, Y, X, D = 0, 4, 8, 12
LAST = [OWN + 2, OWN, OWN + 3, OWN + 1]
ORDER = [
    [Y + 2, X, Y + 3, X + 1, D, D + 2, D + 1, D + 3, Y, X + 2, Y + 1, X + 3] + LAST,
    [Y + 2, Y + 3, D, X, D + 2, D + 1, D + 3, X + 1, X + 2, Y, X + 3, Y + 1] + LAST,
    [X, X + 1, D + 2, Y + 2, D, D + 3, D + 1, Y + 3, Y, X + 2, Y + 1, X + 3] + LAST,
    [D, D + 2, D + 1, D + 3, X, Y + 2, X + 1, Y + 3, X + 2, Y, X + 3, Y + 1] + LAST,
]
EARLY = [4, 2, 2, 4]
_OWNED = [4 * core + quarter for core in range(2) for quarter in (0, 2, 1, 3)]
_FIRST = [u for a, b in ((18, 8), (19, 9)) for u in (a, b, a + 4, b + 4)]
_SECOND = [u for a, b in ((16, 10), (17, 11)) for u in (a, b, a + 4, b + 4)]
_ACROSS = [u for a, b in ((24, 26), (25, 27)) for u in (a, b, a + 4, b + 4)]
LANDING = [_OWNED + _FIRST + _SECOND + _ACROSS, _OWNED + _FIRST + _ACROSS + _SECOND]


def _choose(i, values):
    out = jnp.int32(values[-1])
    for n, value in enumerate(values[:-1]):
        out = jnp.where(i == n, jnp.int32(value), out)
    return out


def _packed(row, bits):
    per = 32 // bits
    words = [sum(v << (bits * n) for n, v in enumerate(row[at : at + per])) for at in range(0, len(row), per)]
    return [w - 2**32 if w >= 2**31 else w for w in words]


def _unpacked(i, words, bits):
    per = 32 // bits
    return (_choose(i // per, words) >> (bits * (i % per))) & (2**bits - 1)


def _flip(bit, by):
    return bit + by - 2 * bit * by


def _dot(a, b, ca=1, cb=0):
    return lax.dot_general(a, b, (((ca,), (cb,)), ((), ())), preferred_element_type=F32)


def _kernel(x_hbm, gain_hbm, wq_hbm, wk_hbm, wv_hbm, wo_hbm, coarse_hbm, fine_hbm, out_ref,
            x_s, gain_ref, coarse_ref, fine_ref, wq_s, wk_s, wv_s, wo_s, xg, q_s, k_s, v_s, near_s, far_s, mine_s, o_s, top_s, most_s, mix_s, sa_s, sb_s,
            load_sem, got_sem, core_sem, xs_sem, ys_sem, near_send, near_got, far_send, far_got):
    me = lax.axis_index("tp")
    mx, my, mc = me // 4, (me // 2) % 2, me % 2
    partner, nx, ny = me + 1 - 2 * mc, me + 4 - 8 * mx, me + 2 - 4 * my

    barrier = pltpu.get_barrier_semaphore()
    for other in (partner, nx, ny):
        pl.semaphore_signal(barrier, inc=1, device_id={"tp": other}, device_id_type=pl.DeviceIdType.MESH)
    quarters = [pl.ds(q * UNIT, UNIT) for q in range(4)]
    pairs = [(gain_hbm, gain_ref)] + [(x_hbm.at[quarters[q], :], x_s.at[quarters[q], :]) for q in (0, 2, 1, 3)]
    pairs += [(coarse_hbm, coarse_ref), (fine_hbm, fine_ref), (wq_hbm, wq_s), (wk_hbm, wk_s), (wv_hbm, wv_s), (wo_hbm, wo_s)]
    loads = [pltpu.make_async_copy(a, b, load_sem.at[n]) for n, (a, b) in enumerate(pairs)]
    for load in loads:
        load.start()
    loads[0].wait()
    pl.semaphore_wait(barrier, 3)

    def slot(i, rows):
        return xg.at[pl.ds(pl.multiple_of(i * rows, rows), rows), :]

    def remote(src, dst, send, recv, to):
        return pltpu.make_async_remote_copy(src_ref=src, dst_ref=dst, send_sem=send, recv_sem=recv, device_id={"tp": to},
                                            device_id_type=pl.DeviceIdType.MESH)

    def block_to(u, v, sems, to):
        own = u // 16 * 2 if sems is ys_sem else u // 8 * 4
        return remote(slot(u, UNIT), slot(v, UNIT), sems.at[own + u % 4], got_sem.at[v], to)

    gain = gain_ref[...].reshape(1, -1).astype(F32)

    def norm(i, carry):
        at = pl.ds(pl.multiple_of(i * 32, 32), 32)
        wide = x_s[at, :].astype(F32)
        scale = lax.rsqrt(jnp.mean(wide * wide, -1, keepdims=True) + 1e-6)
        xg[at, :] = (wide * scale * gain).astype(BF16)
        return carry

    chip = 2 * mx + my
    early = _choose(chip, EARLY)

    def send(q, *which):
        for sems, other, by in which:
            block_to(q, q + by, sems, other).start()

    to_core, to_x, to_y = (core_sem, partner, 4), (xs_sem, nx, 16), (ys_sem, ny, 8)
    per = UNIT // 32
    for n, q in enumerate((0, 2, 1, 3)):
        loads[1 + n].wait()
        lax.fori_loop(q * per, (q + 1) * per, norm, 0)
        if q == 0:
            send(0, to_y, to_core)
        elif q == 2:
            send(2, to_x, to_core)
        elif q == 1:
            send(1, to_y, to_core)
        else:
            send(3, to_x, to_core)

            @pl.when(chip != 1)
            def _():
                send(0, to_x)
                send(1, to_x)

            @pl.when(chip != 2)
            def _():
                send(2, to_y)
                send(3, to_y)
    for i in range(2):
        v_s[i, HEAD:, :] = jnp.ones((8, v_s.shape[2]), BF16)
    for load in loads[5:]:
        load.wait()

    sign = jnp.where(lax.broadcasted_iota(jnp.int32, (1, HEAD), 1) < HEAD // 2, -1.0, 1.0).astype(F32)

    strips = [(i, g) for g in range(2) for i in range(2)]
    strip_of = {s: n for n, s in enumerate(strips)}

    orders = [_packed(row, 4) for row in ORDER]
    order = [_choose(chip, [row[n] for row in orders]) for n in range(2)]

    def which(t):
        piece = (jnp.where(t < 8, order[0], order[1]) >> (4 * (t % 8))) & 15
        return piece // 8, (piece // 4) % 2, piece % 4

    bufs = (sa_s, sb_s)

    def score(first, j, n, buf):
        i, g = strips[n]
        keys = pl.ds(pl.multiple_of(j * BK, BK), BK)
        rows = pl.ds(pl.multiple_of(first + g * 512, PIECE), PIECE)
        s = _dot(k_s[i, keys, :], q_s[2 * i : 2 * i + 2, rows, :].reshape(2 * PIECE, HEAD), 1, 1)
        bufs[buf][n] = s
        most_s[4 * buf + n : 4 * buf + n + 1, :] = s.max(axis=0, keepdims=True)

    def absorb(j, n, buf, p, masked):
        i, g = strips[n]
        keys = pl.ds(pl.multiple_of(j * BK, BK), BK)
        s = bufs[buf][n]
        if masked:
            gap = (lax.broadcasted_iota(jnp.int32, (BK, 2 * PIECE), 1) % PIECE) - lax.broadcasted_iota(jnp.int32, (BK, 2 * PIECE), 0)
            s = jnp.where(gap + p * PIECE >= 0, s, HIDDEN)
            most = s.max(axis=0, keepdims=True)
        else:
            most = most_s[4 * buf + n : 4 * buf + n + 1, :]
        old = top_s[n : n + 1, :]
        top = jnp.maximum(old, most)
        top_s[n : n + 1, :] = top
        w = jnp.exp2((s - top) * E).astype(BF16)
        mix_s[n] = mix_s[n] * jnp.exp2((old - top) * E) + _dot(v_s[i, :, keys], w)

    def rows_of(t):
        bx, by, p = which(t)
        there = 2 * _flip(mx, bx) + _flip(my, by)
        return there, there * 1024 + p * PIECE, p

    def begin(t):
        there, first, p = rows_of(t)
        top_s[...] = jnp.full(top_s.shape, NEG, F32)
        mix_s[...] = jnp.zeros(mix_s.shape, F32)
        for n in range(4):
            score(first, 0, n, 0)

        def two(c, carry):
            for buf in range(2):
                for n in range(4):
                    score(first, 2 * c + buf + 1, n, 1 - buf)
                    absorb(2 * c + buf, n, buf, p, False)
            return carry

        lax.fori_loop(0, there, two, 0)

    def again(t):
        there, first, p = rows_of(t)
        for n in range(4):
            score(first, 2 * there, n, 0)

    def end(t):
        there, first, p = rows_of(t)
        for n in (2, 3):
            score(first, 2 * there + 1, n, 1)
        for n in range(4):
            absorb(2 * there, n, 0, p, n < 2)
        for n in (2, 3):
            absorb(2 * there + 1, n, 1, p, True)
        for n, (i, g) in enumerate(strips):
            o = (mix_s[n, :HEAD, :] * (1 / mix_s[n, HEAD : HEAD + 1, :])).T.astype(BF16)
            for m in range(2):
                o_s[g, :, (2 * i + m) * HEAD : (2 * i + m + 1) * HEAD] = o[m * PIECE : (m + 1) * PIECE, :]

    def near_slot(t):
        return jnp.where(t < 4, 4 + t, jnp.where(t < 10, 12 + t, 14 + t))

    def far_slot(t):
        return jnp.where(t < 2, 12 + t, jnp.where(t < 4, 20 + t, jnp.where(t < 8, t - 4, t)))

    def near(t):
        return remote(slot(near_slot(t), PIECE), near_s.at[t], near_send.at[t], near_got.at[t], partner)

    def far(t, to_slot, to):
        return remote(slot(far_slot(t), PIECE), far_s.at[to_slot], far_send.at[t], far_got.at[to_slot], to)

    def project(t):
        for n in range(0, 2048, 512):
            slot(near_slot(t), PIECE)[:, n : n + 512] = _dot(o_s[1 - mc], wo_s[:, n : n + 512]).astype(BF16)
        near(t).start()
        for n in range(0, 2048, 512):
            mine_s[jnp.maximum(t - 11, 0), :, n : n + 512] = _dot(o_s[mc], wo_s[:, n : n + 512])

    def tiles(body):
        def step(i, carry):
            body(pl.ds(pl.multiple_of(i * 32, 32), 32), i * 32)
            return carry

        lax.fori_loop(0, PIECE // 32, step, 0)

    def finish(t):
        bx, by, p = which(t)
        low = p < 2
        near(t).wait_recv()
        summed = ((by == 0) & jnp.logical_not(low)) | ((bx == 0) & low)

        @pl.when(summed)
        def _():
            far(0, p, nx).wait_recv()

            def body(at, i):
                to = pl.ds(pl.multiple_of(far_slot(t) * PIECE + i, 32), 32)
                xg[to, :] = (mine_s[0, at, :] + near_s[t, at, :].astype(F32) + far_s[p, at, :].astype(F32)).astype(BF16)

            tiles(body)

        @pl.when(jnp.logical_not(summed))
        def _():
            def body(at, i):
                to = pl.ds(pl.multiple_of(far_slot(t) * PIECE + i, 32), 32)
                xg[to, :] = (mine_s[0, at, :] + near_s[t, at, :].astype(F32)).astype(BF16)

            tiles(body)

        to_slot = p + 4 * bx * (1 - by) + 8 * by * (1 - bx)
        along_x = (by == 0) | ((bx == 1) & low)

        @pl.when(along_x)
        def _():
            far(t, to_slot, nx).start()

        @pl.when(jnp.logical_not(along_x))
        def _():
            far(t, to_slot, ny).start()

    def conclude(t, carry):
        p = which(t)[2]
        near(t).wait_recv()
        far(0, 4 + p, nx).wait_recv()
        far(0, 8 + p, ny).wait_recv()

        def body(at, i):
            to = pl.ds(pl.multiple_of(p * PIECE + i, 32), 32)
            total = mine_s[t - 11, at, :] + near_s[t, at, :].astype(F32)
            total = total + far_s[4 + p, at, :].astype(F32) + far_s[8 + p, at, :].astype(F32)
            out_ref[to, :] = (x_s[to, :].astype(F32) + total).astype(BF16)

        tiles(body)
        return carry

    def ahead_of_time(t, carry):
        begin(t)
        end(t)
        project(t)
        finish(t)
        return carry

    def landed(n, carry):
        ahead = jnp.minimum(early, 2)
        first = jnp.where(n == 28, ahead, 0)
        lax.fori_loop(first, jnp.where(n == 24, ahead, jnp.where(n == 28, early, 0)), ahead_of_time, 0)

        @pl.when((n == 28) & (early == 2))
        def _():
            begin(early)

        u = jnp.where(chip == 3, *(_unpacked(n, _packed(row, 8), 8) for row in LANDING[::-1]))
        bx, by, bc, quarter = u // 16, (u // 8) % 2, (u // 4) % 2, u % 4

        @pl.when(bx + by + bc > 0)
        def _():
            block_to(u, u, core_sem, partner).wait_recv()

        @pl.when((bc == 0) & (bx + by > 0))
        def _():
            block_to(u, u + 4, core_sem, partner).start()

        @pl.when((bc == 0) & (by == 1) & (bx == 0) & (quarter < 2))
        def _():
            block_to(u, 24 + quarter, xs_sem, nx).start()

            @pl.when((chip == 1) & (quarter == 1))
            def _():
                send(0, to_x)
                send(1, to_x)

        @pl.when((bc == 0) & (by == 0) & (bx == 1) & (quarter >= 2))
        def _():
            block_to(u, 24 + quarter, ys_sem, ny).start()

            @pl.when((chip == 2) & (quarter == 3))
            def _():
                send(2, to_y)
                send(3, to_y)

        place = (4 * _flip(mx, bx) + 2 * _flip(my, by) + _flip(mc, bc)) * 4 + quarter
        rows = pl.ds(pl.multiple_of(place * UNIT, UNIT), UNIT)
        base = coarse_ref[pl.ds(place, 1), :]
        cos_a, sin_a = base[:, :HEAD], base[:, HEAD:]
        cos_b, sin_b = fine_ref[:, :HEAD], fine_ref[:, HEAD:]
        cos = cos_a * cos_b - sin_a * sin_b
        sin = (sin_a * cos_b + cos_a * sin_b) * sign

        def turned(t):
            t = t.astype(BF16).astype(F32)
            return (t * cos + pltpu.roll(t, HEAD // 2, 1) * sin).astype(BF16)

        a = slot(u, UNIT)
        q = _dot(a[...], wq_s[...])
        for i in range(4):
            q_s[i, rows, :] = turned(q[:, i * HEAD : (i + 1) * HEAD])
        k = _dot(a[...], wk_s[...])
        for i in range(2):
            k_s[i, rows, :] = turned(k[:, i * HEAD : (i + 1) * HEAD])
        v = _dot(a[...], wv_s[...])
        for i in range(2):
            v_s[i, :HEAD, rows] = v[:, i * HEAD : (i + 1) * HEAD].T.astype(BF16)
        return carry

    lax.fori_loop(0, 32, landed, 0)
    for r in (0, 8, 16, 24):
        for q in range(4):
            block_to(r + q, r + q + 4, core_sem, partner).wait_send()
    for u in (0, 1, 2, 3, 8, 9):
        block_to(u, u, xs_sem, nx).wait_send()
    for u in (0, 1, 2, 3, 18, 19):
        block_to(u, u, ys_sem, ny).wait_send()

    def piece(t, carry):
        soon = (early == 2) & (t == 3)

        @pl.when(soon)
        def _():
            finish(t - 1)

        begun = (early == 2) & (t == 2)

        @pl.when(begun)
        def _():
            again(t)

        @pl.when(jnp.logical_not(begun))
        def _():
            begin(t)

        end(t)

        @pl.when(jnp.logical_not(soon) & (t > early) & (t <= 12))
        def _():
            finish(t - 1)

        project(t)
        return carry

    lax.fori_loop(early, 16, piece, 0)
    lax.fori_loop(12, 16, conclude, 0)

    def sent(t, carry):
        near(t).wait_send()

        @pl.when(t < 12)
        def _():
            far(t, 0, nx).wait_send()

        return carry

    lax.fori_loop(0, 16, sent, 0)


def tables():
    half = HEAD // 2
    rate = np.concatenate([float(THETA) ** (-np.arange(half) / half)] * 2)
    a = np.arange(32)[:, None] * UNIT * rate
    b = np.arange(UNIT)[:, None] * rate
    both = lambda t: np.concatenate([np.cos(t), np.sin(t)], 1).astype(np.float32)
    return both(a), both(b)


def solution(mesh):
    def step(x, gain, wq, wk, wv, wo):
        rows, d = x.shape
        group = rows * 8
        coarse, fine = tables()
        hbm, vmem = pl.BlockSpec(memory_space=pl.ANY), pl.BlockSpec(memory_space=pltpu.VMEM)
        dma = pltpu.SemaphoreType.DMA
        return pl.pallas_call(
            _kernel,
            out_shape=pltpu.VMEM((rows, d), BF16),
            in_specs=[hbm] * 8,
            out_specs=vmem,
            scratch_shapes=[
                pltpu.VMEM(x.shape, BF16), pltpu.VMEM(gain.shape, BF16), pltpu.VMEM(coarse.shape, F32), pltpu.VMEM(fine.shape, F32),
                pltpu.VMEM(wq.shape, BF16), pltpu.VMEM(wk.shape, BF16), pltpu.VMEM(wv.shape, BF16),
                pltpu.VMEM(wo.shape, BF16),
                pltpu.VMEM((group, d), BF16),
                pltpu.VMEM((4, group, HEAD), BF16), pltpu.VMEM((2, group, HEAD), BF16), pltpu.VMEM((2, HEAD + 8, group), BF16),
                pltpu.VMEM((16, PIECE, d), BF16), pltpu.VMEM((12, PIECE, d), BF16), pltpu.VMEM((5, PIECE, d), F32),
                pltpu.VMEM((2, PIECE, 4 * HEAD), BF16), pltpu.VMEM((8, 2 * PIECE), F32), pltpu.VMEM((8, 2 * PIECE), F32), pltpu.VMEM((4, HEAD + 8, 2 * PIECE), F32),
                pltpu.VMEM((4, BK, 2 * PIECE), F32), pltpu.VMEM((4, BK, 2 * PIECE), F32),
                dma((11,)), dma((32,)), dma((16,)), dma((6,)), dma((6,)), dma((16,)), dma((16,)), dma((12,)), dma((12,)),
            ],
            compiler_params=pltpu.CompilerParams(collective_id=0, has_side_effects=True, vmem_limit_bytes=60 * 2**20),
        )(x, gain, wq, wk, wv, wo, jnp.asarray(coarse), jnp.asarray(fine))

    tokens, columns = P(("dp", "tp"), None), P(None, "tp")
    return jax.shard_map(
        step,
        mesh=mesh,
        in_specs=(tokens, P(None), columns, columns, columns, P("tp", None)),
        out_specs=tokens,
        check_vma=False,
    )
```

```python
import functools

import jax
import jax.numpy as jnp
import numpy as np
from jax import lax
from jax.experimental import pallas as pl
from jax.experimental.pallas import tpu as pltpu
from jax.sharding import PartitionSpec as P

HEAD = 128
THETA = 10000
NEG = -1e30
HIDDEN = 2 * NEG
LOG2E = 1.4426950408889634
E = HEAD**-0.5 * LOG2E
UNIT = 128
PIECE = 128
BK = 512
F32, BF16 = jnp.float32, jnp.bfloat16

OWN, Y, X, D = 0, 4, 8, 12
LAST = [OWN + 2, OWN, OWN + 3, OWN + 1]
ORDER = [
    [Y + 2, X, Y + 3, X + 1, D, D + 2, D + 1, D + 3, Y, X + 2, Y + 1, X + 3] + LAST,
    [Y + 2, Y + 3, D, X, D + 2, D + 1, D + 3, X + 1, X + 2, Y, X + 3, Y + 1] + LAST,
    [X, X + 1, D + 2, Y + 2, D, D + 3, D + 1, Y + 3, Y, X + 2, Y + 1, X + 3] + LAST,
    [D, D + 2, D + 1, D + 3, X, Y + 2, X + 1, Y + 3, X + 2, Y, X + 3, Y + 1] + LAST,
]
EARLY = [4, 2, 2, 4]
_OWNED = [4 * core + quarter for core in range(2) for quarter in (0, 2, 1, 3)]
_FIRST = [u for a, b in ((18, 8), (19, 9)) for u in (a, b, a + 4, b + 4)]
_SECOND = [u for a, b in ((16, 10), (17, 11)) for u in (a, b, a + 4, b + 4)]
_ACROSS = [u for a, b in ((24, 26), (25, 27)) for u in (a, b, a + 4, b + 4)]
LANDING = [_OWNED + _FIRST + _SECOND + _ACROSS, _OWNED + _FIRST + _ACROSS + _SECOND]


def _choose(i, values):
    out = jnp.int32(values[-1])
    for n, value in enumerate(values[:-1]):
        out = jnp.where(i == n, jnp.int32(value), out)
    return out


def _packed(row, bits):
    per = 32 // bits
    words = [sum(v << (bits * n) for n, v in enumerate(row[at : at + per])) for at in range(0, len(row), per)]
    return [w - 2**32 if w >= 2**31 else w for w in words]


def _unpacked(i, words, bits):
    per = 32 // bits
    return (_choose(i // per, words) >> (bits * (i % per))) & (2**bits - 1)


def _flip(bit, by):
    return bit + by - 2 * bit * by


def _dot(a, b, ca=1, cb=0):
    return lax.dot_general(a, b, (((ca,), (cb,)), ((), ())), preferred_element_type=F32)


def _kernel(x_hbm, gain_hbm, wq_hbm, wk_hbm, wv_hbm, wo_hbm, coarse_hbm, fine_hbm, out_ref,
            x_s, gain_ref, coarse_ref, fine_ref, wq_s, wk_s, wv_s, wo_s, xg, q_s, k_s, v_s, near_s, far_s, mine_s, o_s, top_s, most_s, mix_s, sa_s, sb_s,
            load_sem, got_sem, core_sem, xs_sem, ys_sem, near_send, near_got, far_send, far_got):
    me = lax.axis_index("tp")
    mx, my, mc = me // 4, (me // 2) % 2, me % 2
    partner, nx, ny = me + 1 - 2 * mc, me + 4 - 8 * mx, me + 2 - 4 * my

    barrier = pltpu.get_barrier_semaphore()
    for other in (partner, nx, ny):
        pl.semaphore_signal(barrier, inc=1, device_id={"tp": other}, device_id_type=pl.DeviceIdType.MESH)
    quarters = [pl.ds(q * UNIT, UNIT) for q in range(4)]
    pairs = [(gain_hbm, gain_ref)] + [(x_hbm.at[quarters[q], :], x_s.at[quarters[q], :]) for q in (0, 2, 1, 3)]
    pairs += [(coarse_hbm, coarse_ref), (fine_hbm, fine_ref), (wq_hbm, wq_s), (wk_hbm, wk_s), (wv_hbm, wv_s), (wo_hbm, wo_s)]
    loads = [pltpu.make_async_copy(a, b, load_sem.at[n]) for n, (a, b) in enumerate(pairs)]
    for load in loads:
        load.start()
    loads[0].wait()
    pl.semaphore_wait(barrier, 3)

    def slot(i, rows):
        return xg.at[pl.ds(pl.multiple_of(i * rows, rows), rows), :]

    def remote(src, dst, send, recv, to):
        return pltpu.make_async_remote_copy(src_ref=src, dst_ref=dst, send_sem=send, recv_sem=recv, device_id={"tp": to},
                                            device_id_type=pl.DeviceIdType.MESH)

    def block_to(u, v, sems, to):
        own = u // 16 * 2 if sems is ys_sem else u // 8 * 4
        return remote(slot(u, UNIT), slot(v, UNIT), sems.at[own + u % 4], got_sem.at[v], to)

    gain = gain_ref[...].reshape(1, -1).astype(F32)

    def norm(i, carry):
        at = pl.ds(pl.multiple_of(i * 32, 32), 32)
        wide = x_s[at, :].astype(F32)
        scale = lax.rsqrt(jnp.mean(wide * wide, -1, keepdims=True) + 1e-6)
        xg[at, :] = (wide * scale * gain).astype(BF16)
        return carry

    chip = 2 * mx + my
    early = _choose(chip, EARLY)

    def send(q, *which):
        for sems, other, by in which:
            block_to(q, q + by, sems, other).start()

    to_core, to_x, to_y = (core_sem, partner, 4), (xs_sem, nx, 16), (ys_sem, ny, 8)
    per = UNIT // 32
    for n, q in enumerate((0, 2, 1, 3)):
        loads[1 + n].wait()
        lax.fori_loop(q * per, (q + 1) * per, norm, 0)
        if q == 0:
            send(0, to_y, to_core)
        elif q == 2:
            send(2, to_x, to_core)
        elif q == 1:
            send(1, to_y, to_core)
        else:
            send(3, to_x, to_core)

            @pl.when(chip != 1)
            def _():
                send(0, to_x)
                send(1, to_x)

            @pl.when(chip != 2)
            def _():
                send(2, to_y)
                send(3, to_y)
    for i in range(2):
        v_s[i, HEAD:, :] = jnp.ones((8, v_s.shape[2]), BF16)
    for load in loads[5:]:
        load.wait()

    sign = jnp.where(lax.broadcasted_iota(jnp.int32, (1, HEAD), 1) < HEAD // 2, -1.0, 1.0).astype(F32)

    strips = [(i, g) for g in range(2) for i in range(2)]
    strip_of = {s: n for n, s in enumerate(strips)}

    orders = [_packed(row, 4) for row in ORDER]
    order = [_choose(chip, [row[n] for row in orders]) for n in range(2)]

    def which(t):
        piece = (jnp.where(t < 8, order[0], order[1]) >> (4 * (t % 8))) & 15
        return piece // 8, (piece // 4) % 2, piece % 4

    bufs = (sa_s, sb_s)

    def score(first, j, n, buf, many=BK):
        i, g = strips[n]
        keys = pl.ds(pl.multiple_of(j * BK, BK), many)
        rows = pl.ds(pl.multiple_of(first + g * 512, PIECE), PIECE)
        s = _dot(k_s[i, keys, :], q_s[2 * i : 2 * i + 2, rows, :].reshape(2 * PIECE, HEAD), 1, 1)
        bufs[buf][n, :many, :] = s
        most_s[4 * buf + n : 4 * buf + n + 1, :] = s.max(axis=0, keepdims=True)

    def absorb(j, n, buf, p, masked, many=BK):
        i, g = strips[n]
        keys = pl.ds(pl.multiple_of(j * BK, BK), many)
        s = bufs[buf][n, :many, :]
        if masked:
            query = lax.broadcasted_iota(jnp.int32, s.shape, 1) % PIECE + p * PIECE
            s = jnp.where(query >= lax.broadcasted_iota(jnp.int32, s.shape, 0), s, HIDDEN)
            most = s.max(axis=0, keepdims=True)
        else:
            most = most_s[4 * buf + n : 4 * buf + n + 1, :]
        old = top_s[n : n + 1, :]
        top = jnp.maximum(old, most)
        top_s[n : n + 1, :] = top
        w = jnp.exp2((s - top) * E).astype(BF16)
        mix_s[n] = mix_s[n] * jnp.exp2((old - top) * E) + _dot(v_s[i, :, keys], w)

    def rows_of(t):
        bx, by, p = which(t)
        there = 2 * _flip(mx, bx) + _flip(my, by)
        return there, there * 1024 + p * PIECE, p

    def begin(t):
        there, first, p = rows_of(t)
        top_s[...] = jnp.full(top_s.shape, NEG, F32)
        mix_s[...] = jnp.zeros(mix_s.shape, F32)
        for n in range(4):
            score(first, 0, n, 0)

        def two(c, carry):
            for buf in range(2):
                for n in range(4):
                    score(first, 2 * c + buf + 1, n, 1 - buf)
                    absorb(2 * c + buf, n, buf, p, False)
            return carry

        lax.fori_loop(0, there, two, 0)

    def again(t):
        there, first, p = rows_of(t)
        for n in range(4):
            score(first, 2 * there, n, 0)

    def end(t):
        there, first, p = rows_of(t)
        def cut(many):
            for n in (2, 3):
                score(first, 2 * there + 1, n, 1, many)
            for n in (2, 3, 0, 1):
                absorb(2 * there, n, 0, p, n < 2, many if n < 2 else BK)
            for n in (2, 3):
                absorb(2 * there + 1, n, 1, p, True, many)

        @pl.when(p < 2)
        def _():
            cut(BK // 2)

        @pl.when(p >= 2)
        def _():
            cut(BK)

        for n, (i, g) in enumerate(strips):
            o = (mix_s[n, :HEAD, :] * (1 / mix_s[n, HEAD : HEAD + 1, :])).T.astype(BF16)
            for m in range(2):
                o_s[g, :, (2 * i + m) * HEAD : (2 * i + m + 1) * HEAD] = o[m * PIECE : (m + 1) * PIECE, :]

    def near_slot(t):
        return jnp.where(t < 4, 4 + t, jnp.where(t < 10, 12 + t, 14 + t))

    def far_slot(t):
        return jnp.where(t < 2, 12 + t, jnp.where(t < 4, 20 + t, jnp.where(t < 8, t - 4, t)))

    def near(t):
        return remote(slot(near_slot(t), PIECE), near_s.at[t], near_send.at[t], near_got.at[t], partner)

    def far(t, to_slot, to):
        return remote(slot(far_slot(t), PIECE), far_s.at[to_slot], far_send.at[t], far_got.at[to_slot], to)

    def project(t):
        for n in range(0, 2048, 512):
            slot(near_slot(t), PIECE)[:, n : n + 512] = _dot(o_s[1 - mc], wo_s[:, n : n + 512]).astype(BF16)
        near(t).start()
        for n in range(0, 2048, 512):
            mine_s[jnp.maximum(t - 11, 0), :, n : n + 512] = _dot(o_s[mc], wo_s[:, n : n + 512])

    def tiles(body):
        def step(i, carry):
            body(pl.ds(pl.multiple_of(i * 32, 32), 32), i * 32)
            return carry

        lax.fori_loop(0, PIECE // 32, step, 0)

    def finish(t):
        bx, by, p = which(t)
        low = p < 2
        near(t).wait_recv()
        summed = ((by == 0) & jnp.logical_not(low)) | ((bx == 0) & low)

        @pl.when(summed)
        def _():
            far(0, p, nx).wait_recv()

            def body(at, i):
                to = pl.ds(pl.multiple_of(far_slot(t) * PIECE + i, 32), 32)
                xg[to, :] = (mine_s[0, at, :] + near_s[t, at, :].astype(F32) + far_s[p, at, :].astype(F32)).astype(BF16)

            tiles(body)

        @pl.when(jnp.logical_not(summed))
        def _():
            def body(at, i):
                to = pl.ds(pl.multiple_of(far_slot(t) * PIECE + i, 32), 32)
                xg[to, :] = (mine_s[0, at, :] + near_s[t, at, :].astype(F32)).astype(BF16)

            tiles(body)

        to_slot = p + 4 * bx * (1 - by) + 8 * by * (1 - bx)
        along_x = (by == 0) | ((bx == 1) & low)

        @pl.when(along_x)
        def _():
            far(t, to_slot, nx).start()

        @pl.when(jnp.logical_not(along_x))
        def _():
            far(t, to_slot, ny).start()

    def conclude(t, carry):
        p = which(t)[2]
        near(t).wait_recv()
        far(0, 4 + p, nx).wait_recv()
        far(0, 8 + p, ny).wait_recv()

        def body(at, i):
            to = pl.ds(pl.multiple_of(p * PIECE + i, 32), 32)
            total = mine_s[t - 11, at, :] + near_s[t, at, :].astype(F32)
            total = total + far_s[4 + p, at, :].astype(F32) + far_s[8 + p, at, :].astype(F32)
            out_ref[to, :] = (x_s[to, :].astype(F32) + total).astype(BF16)

        tiles(body)
        return carry

    def ahead_of_time(t, carry):
        begin(t)
        end(t)
        project(t)
        finish(t)
        return carry

    def landed(n, carry):
        ahead = jnp.minimum(early, 2)
        first = jnp.where(n == 28, ahead, 0)
        lax.fori_loop(first, jnp.where(n == 24, ahead, jnp.where(n == 28, early, 0)), ahead_of_time, 0)

        @pl.when((n == 28) & (early == 2))
        def _():
            begin(early)

        u = jnp.where(chip == 3, *(_unpacked(n, _packed(row, 8), 8) for row in LANDING[::-1]))
        bx, by, bc, quarter = u // 16, (u // 8) % 2, (u // 4) % 2, u % 4

        def relay(u):
            block_to(u, u, core_sem, partner).wait_recv()
            block_to(u, u + 4, core_sem, partner).start()

        last_two = (n == 28) | (n == 29)

        @pl.when(bc == 1)
        def _():
            block_to(u, u, core_sem, partner).wait_recv()

        @pl.when((bc == 0) & (bx + by > 0) & jnp.logical_not(last_two))
        def _():
            relay(u)

        @pl.when(n == 28)
        def _():
            relay(u)
            relay(jnp.where(chip == 3, LANDING[1][29], LANDING[0][29]))

        @pl.when((bc == 0) & (by == 1) & (bx == 0) & (quarter < 2))
        def _():
            block_to(u, 24 + quarter, xs_sem, nx).start()

            @pl.when((chip == 1) & (quarter == 1))
            def _():
                send(0, to_x)
                send(1, to_x)

        @pl.when((bc == 0) & (by == 0) & (bx == 1) & (quarter >= 2))
        def _():
            block_to(u, 24 + quarter, ys_sem, ny).start()

            @pl.when((chip == 2) & (quarter == 3))
            def _():
                send(2, to_y)
                send(3, to_y)

        place = (4 * _flip(mx, bx) + 2 * _flip(my, by) + _flip(mc, bc)) * 4 + quarter
        rows = pl.ds(pl.multiple_of(place * UNIT, UNIT), UNIT)
        base = coarse_ref[pl.ds(place, 1), :]
        cos_a, sin_a = base[:, :HEAD], base[:, HEAD:]
        cos_b, sin_b = fine_ref[:, :HEAD], fine_ref[:, HEAD:]
        cos = cos_a * cos_b - sin_a * sin_b
        sin = (sin_a * cos_b + cos_a * sin_b) * sign

        def turned(t):
            t = t.astype(BF16).astype(F32)
            return (t * cos + pltpu.roll(t, HEAD // 2, 1) * sin).astype(BF16)

        a = slot(u, UNIT)
        q = _dot(a[...], wq_s[...])
        for i in range(4):
            q_s[i, rows, :] = turned(q[:, i * HEAD : (i + 1) * HEAD])
        k = _dot(a[...], wk_s[...])
        for i in range(2):
            k_s[i, rows, :] = turned(k[:, i * HEAD : (i + 1) * HEAD])
        v = _dot(a[...], wv_s[...])
        for i in range(2):
            v_s[i, :HEAD, rows] = v[:, i * HEAD : (i + 1) * HEAD].T.astype(BF16)
        return carry

    lax.fori_loop(0, 32, landed, 0)
    for r in (0, 8, 16, 24):
        for q in range(4):
            block_to(r + q, r + q + 4, core_sem, partner).wait_send()
    for u in (0, 1, 2, 3, 8, 9):
        block_to(u, u, xs_sem, nx).wait_send()
    for u in (0, 1, 2, 3, 18, 19):
        block_to(u, u, ys_sem, ny).wait_send()

    def piece(t, carry):
        soon = (early == 2) & (t == 3)

        @pl.when(soon)
        def _():
            finish(t - 1)

        begun = (early == 2) & (t == 2)

        @pl.when(begun)
        def _():
            again(t)

        @pl.when(jnp.logical_not(begun))
        def _():
            begin(t)

        late = jnp.logical_not(soon) & (t > early) & (t <= 12)
        covered = rows_of(t)[0] > 0

        @pl.when(late & covered)
        def _():
            finish(t - 1)

        end(t)

        @pl.when(late & jnp.logical_not(covered))
        def _():
            finish(t - 1)

        project(t)
        return carry

    lax.fori_loop(early, 16, piece, 0)
    lax.fori_loop(12, 16, conclude, 0)

    def sent(t, carry):
        near(t).wait_send()

        @pl.when(t < 12)
        def _():
            far(t, 0, nx).wait_send()

        return carry

    lax.fori_loop(0, 16, sent, 0)


def tables():
    half = HEAD // 2
    rate = np.concatenate([float(THETA) ** (-np.arange(half) / half)] * 2)
    a = np.arange(32)[:, None] * UNIT * rate
    b = np.arange(UNIT)[:, None] * rate
    both = lambda t: np.concatenate([np.cos(t), np.sin(t)], 1).astype(np.float32)
    return both(a), both(b)


def solution(mesh):
    def step(x, gain, wq, wk, wv, wo):
        rows, d = x.shape
        group = rows * 8
        coarse, fine = tables()
        hbm, vmem = pl.BlockSpec(memory_space=pl.ANY), pl.BlockSpec(memory_space=pltpu.VMEM)
        dma = pltpu.SemaphoreType.DMA
        return pl.pallas_call(
            _kernel,
            out_shape=pltpu.VMEM((rows, d), BF16),
            in_specs=[hbm] * 8,
            out_specs=vmem,
            scratch_shapes=[
                pltpu.VMEM(x.shape, BF16), pltpu.VMEM(gain.shape, BF16), pltpu.VMEM(coarse.shape, F32), pltpu.VMEM(fine.shape, F32),
                pltpu.VMEM(wq.shape, BF16), pltpu.VMEM(wk.shape, BF16), pltpu.VMEM(wv.shape, BF16),
                pltpu.VMEM(wo.shape, BF16),
                pltpu.VMEM((group, d), BF16),
                pltpu.VMEM((4, group, HEAD), BF16), pltpu.VMEM((2, group, HEAD), BF16), pltpu.VMEM((2, HEAD + 8, group), BF16),
                pltpu.VMEM((16, PIECE, d), BF16), pltpu.VMEM((12, PIECE, d), BF16), pltpu.VMEM((5, PIECE, d), F32),
                pltpu.VMEM((2, PIECE, 4 * HEAD), BF16), pltpu.VMEM((8, 2 * PIECE), F32), pltpu.VMEM((8, 2 * PIECE), F32), pltpu.VMEM((4, HEAD + 8, 2 * PIECE), F32),
                pltpu.VMEM((4, BK, 2 * PIECE), F32), pltpu.VMEM((4, BK, 2 * PIECE), F32),
                dma((11,)), dma((32,)), dma((16,)), dma((6,)), dma((6,)), dma((16,)), dma((16,)), dma((12,)), dma((12,)),
            ],
            compiler_params=pltpu.CompilerParams(collective_id=0, has_side_effects=True, vmem_limit_bytes=60 * 2**20),
        )(x, gain, wq, wk, wv, wo, jnp.asarray(coarse), jnp.asarray(fine))

    tokens, columns = P(("dp", "tp"), None), P(None, "tp")
    return jax.shard_map(
        step,
        mesh=mesh,
        in_specs=(tokens, P(None), columns, columns, columns, P("tp", None)),
        out_specs=tokens,
        check_vma=False,
    )
```

```python
import functools

import jax
import jax.numpy as jnp
import numpy as np
from jax import lax
from jax.experimental import pallas as pl
from jax.experimental.pallas import tpu as pltpu
from jax.sharding import PartitionSpec as P

HEAD = 128
THETA = 10000
NEG = -1e30
HIDDEN = 2 * NEG
LOG2E = 1.4426950408889634
E = HEAD**-0.5 * LOG2E
UNIT = 128
PIECE = 128
BK = 512
F32, BF16 = jnp.float32, jnp.bfloat16

OWN, Y, X, D = 0, 4, 8, 12
LAST = [OWN + 2, OWN, OWN + 3, OWN + 1]
ORDER = [
    [Y + 2, X, Y + 3, X + 1, D, D + 2, D + 1, D + 3, Y, X + 2, Y + 1, X + 3] + LAST,
    [Y + 2, Y + 3, D, X, D + 2, D + 1, D + 3, X + 1, X + 2, Y, X + 3, Y + 1] + LAST,
    [X, X + 1, D + 2, Y + 2, D, D + 3, D + 1, Y + 3, Y, X + 2, Y + 1, X + 3] + LAST,
    [D, D + 2, D + 1, D + 3, X, Y + 2, X + 1, Y + 3, X + 2, Y, X + 3, Y + 1] + LAST,
]
EARLY = [4, 2, 2, 4]
_OWNED = [4 * core + quarter for core in range(2) for quarter in (0, 2, 1, 3)]
_FIRST = [u for a, b in ((18, 8), (19, 9)) for u in (a, b, a + 4, b + 4)]
_SECOND = [u for a, b in ((16, 10), (17, 11)) for u in (a, b, a + 4, b + 4)]
_ACROSS = [u for a, b in ((24, 26), (25, 27)) for u in (a, b, a + 4, b + 4)]
LANDING = [_OWNED + _FIRST + _SECOND + _ACROSS, _OWNED + _FIRST + _ACROSS + _SECOND]


def _choose(i, values):
    out = jnp.int32(values[-1])
    for n, value in enumerate(values[:-1]):
        out = jnp.where(i == n, jnp.int32(value), out)
    return out


def _packed(row, bits):
    per = 32 // bits
    words = [sum(v << (bits * n) for n, v in enumerate(row[at : at + per])) for at in range(0, len(row), per)]
    return [w - 2**32 if w >= 2**31 else w for w in words]


def _unpacked(i, words, bits):
    per = 32 // bits
    return (_choose(i // per, words) >> (bits * (i % per))) & (2**bits - 1)


def _flip(bit, by):
    return bit + by - 2 * bit * by


def _dot(a, b, ca=1, cb=0):
    return lax.dot_general(a, b, (((ca,), (cb,)), ((), ())), preferred_element_type=F32)


def _kernel(x_hbm, gain_hbm, wq_hbm, wk_hbm, wv_hbm, wo_hbm, coarse_hbm, fine_hbm, out_ref,
            x_s, gain_ref, coarse_ref, fine_ref, wq_s, wk_s, wv_s, wo_s, xg, q_s, k_s, v_s, near_s, far_s, mine_s, o_s, top_s, most_s, mix_s, sa_s, sb_s,
            load_sem, got_sem, core_sem, xs_sem, ys_sem, near_send, near_got, far_send, far_got):
    me = lax.axis_index("tp")
    mx, my, mc = me // 4, (me // 2) % 2, me % 2
    partner, nx, ny = me + 1 - 2 * mc, me + 4 - 8 * mx, me + 2 - 4 * my

    barrier = pltpu.get_barrier_semaphore()
    for other in (partner, nx, ny):
        pl.semaphore_signal(barrier, inc=1, device_id={"tp": other}, device_id_type=pl.DeviceIdType.MESH)
    quarters = [pl.ds(q * UNIT, UNIT) for q in range(4)]
    pairs = [(gain_hbm, gain_ref)] + [(x_hbm.at[quarters[q], :], x_s.at[quarters[q], :]) for q in (0, 2, 1, 3)]
    pairs += [(coarse_hbm, coarse_ref), (fine_hbm, fine_ref), (wq_hbm, wq_s), (wk_hbm, wk_s), (wv_hbm, wv_s), (wo_hbm, wo_s)]
    loads = [pltpu.make_async_copy(a, b, load_sem.at[n]) for n, (a, b) in enumerate(pairs)]
    for load in loads:
        load.start()
    loads[0].wait()
    pl.semaphore_wait(barrier, 3)

    def slot(i, rows):
        return xg.at[pl.ds(pl.multiple_of(i * rows, rows), rows), :]

    def remote(src, dst, send, recv, to):
        return pltpu.make_async_remote_copy(src_ref=src, dst_ref=dst, send_sem=send, recv_sem=recv, device_id={"tp": to},
                                            device_id_type=pl.DeviceIdType.MESH)

    def block_to(u, v, sems, to):
        own = u // 16 * 2 if sems is ys_sem else u // 8 * 4
        return remote(slot(u, UNIT), slot(v, UNIT), sems.at[own + u % 4], got_sem.at[v], to)

    gain = gain_ref[...].reshape(1, -1).astype(F32)

    def norm(i, carry):
        at = pl.ds(pl.multiple_of(i * 32, 32), 32)
        wide = x_s[at, :].astype(F32)
        scale = lax.rsqrt(jnp.mean(wide * wide, -1, keepdims=True) + 1e-6)
        xg[at, :] = (wide * scale * gain).astype(BF16)
        return carry

    chip = 2 * mx + my
    early = _choose(chip, EARLY)

    def send(q, *which):
        for sems, other, by in which:
            block_to(q, q + by, sems, other).start()

    to_core, to_x, to_y = (core_sem, partner, 4), (xs_sem, nx, 16), (ys_sem, ny, 8)
    per = UNIT // 32
    for n, q in enumerate((0, 2, 1, 3)):
        loads[1 + n].wait()
        lax.fori_loop(q * per, (q + 1) * per, norm, 0)
        if q == 0:
            send(0, to_y, to_core)
        elif q == 2:
            send(2, to_x, to_core)
        elif q == 1:
            send(1, to_y, to_core)
        else:
            send(3, to_x, to_core)

            @pl.when(chip != 1)
            def _():
                send(0, to_x)
                send(1, to_x)

            @pl.when(chip != 2)
            def _():
                send(2, to_y)
                send(3, to_y)
    for i in range(2):
        v_s[i, HEAD:, :] = jnp.ones((8, v_s.shape[2]), BF16)
    for load in loads[5:]:
        load.wait()

    sign = jnp.where(lax.broadcasted_iota(jnp.int32, (1, HEAD), 1) < HEAD // 2, -1.0, 1.0).astype(F32)

    strips = [(i, g) for g in range(2) for i in range(2)]
    strip_of = {s: n for n, s in enumerate(strips)}

    orders = [_packed(row, 4) for row in ORDER]
    order = [_choose(chip, [row[n] for row in orders]) for n in range(2)]

    def which(t):
        piece = (jnp.where(t < 8, order[0], order[1]) >> (4 * (t % 8))) & 15
        return piece // 8, (piece // 4) % 2, piece % 4

    bufs = (sa_s, sb_s)

    def score(first, j, n, buf, many=BK):
        i, g = strips[n]
        keys = pl.ds(pl.multiple_of(j * BK, BK), many)
        rows = pl.ds(pl.multiple_of(first + g * 512, PIECE), PIECE)
        s = _dot(k_s[i, keys, :], q_s[2 * i : 2 * i + 2, rows, :].reshape(2 * PIECE, HEAD), 1, 1)
        bufs[buf][n, :many, :] = s
        most_s[4 * buf + n : 4 * buf + n + 1, :] = s.max(axis=0, keepdims=True)

    def absorb(j, n, buf, p, masked, many=BK):
        i, g = strips[n]
        keys = pl.ds(pl.multiple_of(j * BK, BK), many)
        s = bufs[buf][n, :many, :]
        if masked:
            query = lax.broadcasted_iota(jnp.int32, s.shape, 1) % PIECE + p * PIECE
            s = jnp.where(query >= lax.broadcasted_iota(jnp.int32, s.shape, 0), s, HIDDEN)
            most = s.max(axis=0, keepdims=True)
        else:
            most = most_s[4 * buf + n : 4 * buf + n + 1, :]
        old = top_s[n : n + 1, :]
        top = jnp.maximum(old, most)
        top_s[n : n + 1, :] = top
        w = jnp.exp2((s - top) * E).astype(BF16)
        mix_s[n] = mix_s[n] * jnp.exp2((old - top) * E) + _dot(v_s[i, :, keys], w)

    def rows_of(t):
        bx, by, p = which(t)
        there = 2 * _flip(mx, bx) + _flip(my, by)
        return there, there * 1024 + p * PIECE, p

    def begin(t):
        there, first, p = rows_of(t)
        top_s[...] = jnp.full(top_s.shape, NEG, F32)
        mix_s[...] = jnp.zeros(mix_s.shape, F32)
        for n in range(4):
            score(first, 0, n, 0)

        def two(c, carry):
            for buf in range(2):
                for n in range(4):
                    score(first, 2 * c + buf + 1, n, 1 - buf)
                    absorb(2 * c + buf, n, buf, p, False)
            return carry

        lax.fori_loop(0, there, two, 0)

    def again(t):
        there, first, p = rows_of(t)
        for n in range(4):
            score(first, 2 * there, n, 0)

    def end(t):
        there, first, p = rows_of(t)
        def cut(many):
            for n in (2, 3):
                score(first, 2 * there + 1, n, 1, many)
            for n in (2, 3, 0, 1):
                absorb(2 * there, n, 0, p, n < 2, many if n < 2 else BK)
            for n in (2, 3):
                absorb(2 * there + 1, n, 1, p, True, many)

        @pl.when(p < 2)
        def _():
            cut(BK // 2)

        @pl.when(p >= 2)
        def _():
            cut(BK)

        for n, (i, g) in enumerate(strips):
            o = (mix_s[n, :HEAD, :] * (1 / mix_s[n, HEAD : HEAD + 1, :])).T.astype(BF16)
            for m in range(2):
                o_s[g, :, (2 * i + m) * HEAD : (2 * i + m + 1) * HEAD] = o[m * PIECE : (m + 1) * PIECE, :]

    def near_slot(t):
        return jnp.where(t < 4, 4 + t, jnp.where(t < 10, 12 + t, 14 + t))

    def far_slot(t):
        return jnp.where(t < 2, 12 + t, jnp.where(t < 4, 20 + t, jnp.where(t < 8, t - 4, t)))

    def near(t, half):
        columns = pl.ds(half * 1024, 1024)
        return remote(slot(near_slot(t), PIECE).at[:, columns], near_s.at[t, :, columns], near_send.at[2 * t + half], near_got.at[2 * t + half],
                      partner)

    def far(t, to_slot, to):
        return remote(slot(far_slot(t), PIECE), far_s.at[to_slot], far_send.at[t], far_got.at[to_slot], to)

    def project(t):
        for n in range(0, 2048, 512):
            slot(near_slot(t), PIECE)[:, n : n + 512] = _dot(o_s[1 - mc], wo_s[:, n : n + 512]).astype(BF16)
            if n % 1024:
                near(t, n // 1024).start()
        for n in range(0, 2048, 512):
            mine_s[jnp.maximum(t - 11, 0), :, n : n + 512] = _dot(o_s[mc], wo_s[:, n : n + 512])

    def tiles(body):
        def step(i, carry):
            body(pl.ds(pl.multiple_of(i * 32, 32), 32), i * 32)
            return carry

        lax.fori_loop(0, PIECE // 32, step, 0)

    def finish(t):
        bx, by, p = which(t)
        low = p < 2
        near(t, 0).wait_recv()
        near(t, 1).wait_recv()
        summed = ((by == 0) & jnp.logical_not(low)) | ((bx == 0) & low)

        @pl.when(summed)
        def _():
            far(0, p, nx).wait_recv()

            def body(at, i):
                to = pl.ds(pl.multiple_of(far_slot(t) * PIECE + i, 32), 32)
                xg[to, :] = (mine_s[0, at, :] + near_s[t, at, :].astype(F32) + far_s[p, at, :].astype(F32)).astype(BF16)

            tiles(body)

        @pl.when(jnp.logical_not(summed))
        def _():
            def body(at, i):
                to = pl.ds(pl.multiple_of(far_slot(t) * PIECE + i, 32), 32)
                xg[to, :] = (mine_s[0, at, :] + near_s[t, at, :].astype(F32)).astype(BF16)

            tiles(body)

        to_slot = p + 4 * bx * (1 - by) + 8 * by * (1 - bx)
        along_x = (by == 0) | ((bx == 1) & low)

        @pl.when(along_x)
        def _():
            far(t, to_slot, nx).start()

        @pl.when(jnp.logical_not(along_x))
        def _():
            far(t, to_slot, ny).start()

    def conclude(t, carry):
        p = which(t)[2]
        near(t, 0).wait_recv()
        near(t, 1).wait_recv()
        far(0, 4 + p, nx).wait_recv()
        far(0, 8 + p, ny).wait_recv()

        def body(at, i):
            to = pl.ds(pl.multiple_of(p * PIECE + i, 32), 32)
            total = mine_s[t - 11, at, :] + near_s[t, at, :].astype(F32)
            total = total + far_s[4 + p, at, :].astype(F32) + far_s[8 + p, at, :].astype(F32)
            out_ref[to, :] = (x_s[to, :].astype(F32) + total).astype(BF16)

        tiles(body)
        return carry

    def ahead_of_time(t, carry):
        begin(t)
        end(t)
        project(t)
        finish(t)
        return carry

    def landed(n, carry):
        ahead = jnp.minimum(early, 2)
        first = jnp.where(n == 28, ahead, 0)
        lax.fori_loop(first, jnp.where(n == 24, ahead, jnp.where(n == 28, early, 0)), ahead_of_time, 0)

        @pl.when((n == 28) & (early == 2))
        def _():
            begin(early)

        u = jnp.where(chip == 3, *(_unpacked(n, _packed(row, 8), 8) for row in LANDING[::-1]))
        bx, by, bc, quarter = u // 16, (u // 8) % 2, (u // 4) % 2, u % 4

        def relay(u):
            block_to(u, u, core_sem, partner).wait_recv()
            block_to(u, u + 4, core_sem, partner).start()

        last_two = (n == 28) | (n == 29)

        @pl.when(bc == 1)
        def _():
            block_to(u, u, core_sem, partner).wait_recv()

        @pl.when((bc == 0) & (bx + by > 0) & jnp.logical_not(last_two))
        def _():
            relay(u)

        @pl.when(n == 28)
        def _():
            relay(u)
            relay(jnp.where(chip == 3, LANDING[1][29], LANDING[0][29]))

        @pl.when((bc == 0) & (by == 1) & (bx == 0) & (quarter < 2))
        def _():
            block_to(u, 24 + quarter, xs_sem, nx).start()

            @pl.when((chip == 1) & (quarter == 1))
            def _():
                send(0, to_x)
                send(1, to_x)

        @pl.when((bc == 0) & (by == 0) & (bx == 1) & (quarter >= 2))
        def _():
            block_to(u, 24 + quarter, ys_sem, ny).start()

            @pl.when((chip == 2) & (quarter == 3))
            def _():
                send(2, to_y)
                send(3, to_y)

        place = (4 * _flip(mx, bx) + 2 * _flip(my, by) + _flip(mc, bc)) * 4 + quarter
        rows = pl.ds(pl.multiple_of(place * UNIT, UNIT), UNIT)
        base = coarse_ref[pl.ds(place, 1), :]
        cos_a, sin_a = base[:, :HEAD], base[:, HEAD:]
        cos_b, sin_b = fine_ref[:, :HEAD], fine_ref[:, HEAD:]
        cos = cos_a * cos_b - sin_a * sin_b
        sin = (sin_a * cos_b + cos_a * sin_b) * sign

        def turned(t):
            t = t.astype(BF16).astype(F32)
            return (t * cos + pltpu.roll(t, HEAD // 2, 1) * sin).astype(BF16)

        a = slot(u, UNIT)
        q = _dot(a[...], wq_s[...])
        for i in range(4):
            q_s[i, rows, :] = turned(q[:, i * HEAD : (i + 1) * HEAD])
        k = _dot(a[...], wk_s[...])
        for i in range(2):
            k_s[i, rows, :] = turned(k[:, i * HEAD : (i + 1) * HEAD])
        v = _dot(a[...], wv_s[...])
        for i in range(2):
            v_s[i, :HEAD, rows] = v[:, i * HEAD : (i + 1) * HEAD].T.astype(BF16)
        return carry

    lax.fori_loop(0, 32, landed, 0)
    for r in (0, 8, 16, 24):
        for q in range(4):
            block_to(r + q, r + q + 4, core_sem, partner).wait_send()
    for u in (0, 1, 2, 3, 8, 9):
        block_to(u, u, xs_sem, nx).wait_send()
    for u in (0, 1, 2, 3, 18, 19):
        block_to(u, u, ys_sem, ny).wait_send()

    def piece(t, carry):
        soon = (early == 2) & (t == 3)

        @pl.when(soon)
        def _():
            finish(t - 1)

        begun = (early == 2) & (t == 2)

        @pl.when(begun)
        def _():
            again(t)

        @pl.when(jnp.logical_not(begun))
        def _():
            begin(t)

        late = jnp.logical_not(soon) & (t > early) & (t <= 12)
        covered = rows_of(t)[0] > 0

        @pl.when(late & covered)
        def _():
            finish(t - 1)

        end(t)

        @pl.when(late & jnp.logical_not(covered))
        def _():
            finish(t - 1)

        project(t)
        return carry

    lax.fori_loop(early, 16, piece, 0)
    lax.fori_loop(12, 16, conclude, 0)

    def sent(t, carry):
        near(t, 0).wait_send()
        near(t, 1).wait_send()

        @pl.when(t < 12)
        def _():
            far(t, 0, nx).wait_send()

        return carry

    lax.fori_loop(0, 16, sent, 0)


def tables():
    half = HEAD // 2
    rate = np.concatenate([float(THETA) ** (-np.arange(half) / half)] * 2)
    a = np.arange(32)[:, None] * UNIT * rate
    b = np.arange(UNIT)[:, None] * rate
    both = lambda t: np.concatenate([np.cos(t), np.sin(t)], 1).astype(np.float32)
    return both(a), both(b)


def solution(mesh):
    def step(x, gain, wq, wk, wv, wo):
        rows, d = x.shape
        group = rows * 8
        coarse, fine = tables()
        hbm, vmem = pl.BlockSpec(memory_space=pl.ANY), pl.BlockSpec(memory_space=pltpu.VMEM)
        dma = pltpu.SemaphoreType.DMA
        return pl.pallas_call(
            _kernel,
            out_shape=pltpu.VMEM((rows, d), BF16),
            in_specs=[hbm] * 8,
            out_specs=vmem,
            scratch_shapes=[
                pltpu.VMEM(x.shape, BF16), pltpu.VMEM(gain.shape, BF16), pltpu.VMEM(coarse.shape, F32), pltpu.VMEM(fine.shape, F32),
                pltpu.VMEM(wq.shape, BF16), pltpu.VMEM(wk.shape, BF16), pltpu.VMEM(wv.shape, BF16),
                pltpu.VMEM(wo.shape, BF16),
                pltpu.VMEM((group, d), BF16),
                pltpu.VMEM((4, group, HEAD), BF16), pltpu.VMEM((2, group, HEAD), BF16), pltpu.VMEM((2, HEAD + 8, group), BF16),
                pltpu.VMEM((16, PIECE, d), BF16), pltpu.VMEM((12, PIECE, d), BF16), pltpu.VMEM((5, PIECE, d), F32),
                pltpu.VMEM((2, PIECE, 4 * HEAD), BF16), pltpu.VMEM((8, 2 * PIECE), F32), pltpu.VMEM((8, 2 * PIECE), F32), pltpu.VMEM((4, HEAD + 8, 2 * PIECE), F32),
                pltpu.VMEM((4, BK, 2 * PIECE), F32), pltpu.VMEM((4, BK, 2 * PIECE), F32),
                dma((11,)), dma((32,)), dma((16,)), dma((6,)), dma((6,)), dma((32,)), dma((32,)), dma((12,)), dma((12,)),
            ],
            compiler_params=pltpu.CompilerParams(collective_id=0, has_side_effects=True, vmem_limit_bytes=60 * 2**20),
        )(x, gain, wq, wk, wv, wo, jnp.asarray(coarse), jnp.asarray(fine))

    tokens, columns = P(("dp", "tp"), None), P(None, "tp")
    return jax.shard_map(
        step,
        mesh=mesh,
        in_specs=(tokens, P(None), columns, columns, columns, P("tp", None)),
        out_specs=tokens,
        check_vma=False,
    )
```
